32 devices in a mesh: dp: 4 (over y, z), tp: 8 (over x, core).
Axes of the slice: x: 4, y: 2, z: 2, core: 2. Of those that a mesh axis runs over, the one named last changes fastest.
The devices are a block of a 4x4x8 slice.
Arguments:
- y_one: float32 [32, 256, 1280], P('dp', 'tp'), parts along dimension 0
- y_two: float32 [32, 256, 1280], P('dp', 'tp'), parts along dimension 0
- dy_one: float32 [32, 256, 1280], P('dp', 'tp'), parts along dimension 0
- dy_two: float32 [32, 256, 1280], P('dp', 'tp'), parts along dimension 0
- w_qkv: bfloat16 [2, 1280, 16, 3, 80], P(None, None, 'tp')
- w_out: bfloat16 [2, 16, 80, 1280], P(None, 'tp')
- w_up: bfloat16 [2, 1280, 5120], P(None, None, 'tp')
- w_down: bfloat16 [2, 5120, 1280], P(None, 'tp')
Outputs:
- output 1: float32 [32, 256, 1280], P('dp', 'tp'), parts along dimension 0
- output 2: float32 [32, 256, 1280], P('dp', 'tp'), parts along dimension 0
- output 3: float32 [32, 256, 1280], P('dp', 'tp'), parts along dimension 0
- output 4: float32 [32, 256, 1280], P('dp', 'tp'), parts along dimension 0
- output 5: float32 [8, 1280, 16, 3, 80], P('dp', None, 'tp'), parts along dimension 0
- output 6: float32 [8, 16, 80, 1280], P('dp', 'tp'), parts along dimension 0
- output 7: float32 [8, 1280, 5120], P('dp', None, 'tp'), parts along dimension 0
- output 8: float32 [8, 5120, 1280], P('dp', 'tp'), parts along dimension 0
There are 4 independent parts. The reference program is written for one: setup_inputs(seed, part) draws one part's arguments, and reference() takes and returns one part's arrays. A program takes and returns all parts, laid end to end along the dimension named above; an argument that names none is the same for every part.
All inputs are finite; a program needn't handle non-finite values.
Results may differ from the reference program's by a relative error of at most 0.0190658.
Values are sent between devices in bfloat16 or wider.
A program may use at most 768 MiB of HBM per device.

```python
import jax
import jax.numpy as jnp
from jax import lax

SEQ_COUNT = 8
SEQ_LEN = 256
HIDDEN = 1280
N_HEADS = 16
FFN_DIM = 5120
N_LAYERS = 2

HEAD_DIM = HIDDEN // N_HEADS
TOKENS = SEQ_COUNT * SEQ_LEN
STATE_SHAPE = (SEQ_COUNT, SEQ_LEN, HIDDEN)
RMS_EPS = 1e-6
ATTN_SCALE = HEAD_DIM ** -0.5
Q_GAIN = 2.5
OUT_GAIN = 0.6
DOWN_GAIN = 0.5


def setup_inputs(seed: int = 0, part: int = 0) -> dict:
    base_key = jax.random.key(seed)
    act_keys = jax.random.split(jax.random.fold_in(base_key, part), 4)
    w_keys = jax.random.split(jax.random.fold_in(base_key, 100003), 4)
    y_one = jax.random.normal(act_keys[0], STATE_SHAPE, jnp.float32)
    y_two = jax.random.normal(act_keys[1], STATE_SHAPE, jnp.float32)
    dy_one = jax.random.normal(act_keys[2], STATE_SHAPE, jnp.float32)
    dy_two = jax.random.normal(act_keys[3], STATE_SHAPE, jnp.float32)
    qkv_gain = jnp.array([Q_GAIN, 1.0, 1.0], jnp.float32).reshape(1, 1, 1, 3, 1)
    w_qkv = (jax.random.normal(w_keys[0], (N_LAYERS, HIDDEN, N_HEADS, 3, HEAD_DIM), jnp.float32) * qkv_gain * HIDDEN ** -0.5).astype(jnp.bfloat16)
    w_out = (jax.random.normal(w_keys[1], (N_LAYERS, N_HEADS, HEAD_DIM, HIDDEN), jnp.float32) * (OUT_GAIN * HIDDEN ** -0.5)).astype(jnp.bfloat16)
    w_up = (jax.random.normal(w_keys[2], (N_LAYERS, HIDDEN, FFN_DIM), jnp.float32) * HIDDEN ** -0.5).astype(jnp.bfloat16)
    w_down = (jax.random.normal(w_keys[3], (N_LAYERS, FFN_DIM, HIDDEN), jnp.float32) * (DOWN_GAIN * FFN_DIM ** -0.5)).astype(jnp.bfloat16)
    return {"y_one": y_one, "y_two": y_two, "dy_one": dy_one, "dy_two": dy_two, "w_qkv": w_qkv, "w_out": w_out, "w_up": w_up, "w_down": w_down}


def rms_norm(tensor):
    return tensor * lax.rsqrt(jnp.mean(tensor * tensor, axis=-1, keepdims=True) + RMS_EPS)


def rms_back(tensor, grad_in):
    inv_rms = lax.rsqrt(jnp.mean(tensor * tensor, axis=-1, keepdims=True) + RMS_EPS)
    return inv_rms * grad_in - tensor * (inv_rms * inv_rms * inv_rms) * jnp.mean(grad_in * tensor, axis=-1, keepdims=True)


def gelu_tanh(tensor):
    return jax.nn.gelu(tensor, approximate=True)


def mixed_dot(left, right):
    return jnp.dot(left, right, preferred_element_type=jnp.float32)


def as_wide(tensor):
    return tensor.astype(jnp.float32)


def attn_forward(qkv_seq):
    q_heads = as_wide(qkv_seq[0])
    k_heads = as_wide(qkv_seq[1])
    v_heads = as_wide(qkv_seq[2])
    scores = jnp.einsum("nqd,nkd->nqk", q_heads, k_heads) * ATTN_SCALE
    attn_prob = jax.nn.softmax(scores, axis=-1)
    context = jnp.einsum("nqk,nkd->nqd", as_wide(attn_prob.astype(jnp.bfloat16)), v_heads)
    return context.astype(jnp.bfloat16)


def attn_backward(operands):
    qkv_seq, d_context = operands
    q_heads = as_wide(qkv_seq[0])
    k_heads = as_wide(qkv_seq[1])
    v_heads = as_wide(qkv_seq[2])
    scores = jnp.einsum("nqd,nkd->nqk", q_heads, k_heads) * ATTN_SCALE
    attn_prob = jax.nn.softmax(scores, axis=-1)
    d_ctx = as_wide(d_context)
    d_prob = jnp.einsum("nqd,nkd->nqk", d_ctx, v_heads)
    d_value = jnp.einsum("nqk,nqd->nkd", as_wide(attn_prob.astype(jnp.bfloat16)), d_ctx)
    d_scores = attn_prob * (d_prob - jnp.sum(d_prob * attn_prob, axis=-1, keepdims=True)) * ATTN_SCALE
    d_scores = as_wide(d_scores.astype(jnp.bfloat16))
    d_query = jnp.einsum("nqk,nkd->nqd", d_scores, k_heads)
    d_key = jnp.einsum("nqk,nqd->nkd", d_scores, q_heads)
    return jnp.stack([d_query, d_key, d_value]).astype(jnp.bfloat16)


def block_backward(state_in, layer_weights):
    y_one, y_two, dy_one, dy_two = state_in
    w_qkv, w_out, w_up, w_down = layer_weights
    w_qkv_flat = w_qkv.reshape(HIDDEN, 3 * HIDDEN)
    w_out_flat = w_out.reshape(HIDDEN, HIDDEN)
    u_mlp = rms_norm(y_one).astype(jnp.bfloat16).reshape(TOKENS, HIDDEN)
    pre_act = mixed_dot(u_mlp, w_up)
    hidden, gelu_pull = jax.vjp(gelu_tanh, pre_act)
    hidden_b = hidden.astype(jnp.bfloat16)
    x_two = y_two - mixed_dot(hidden_b, w_down).reshape(STATE_SHAPE)
    cot_mlp = dy_two.astype(jnp.bfloat16).reshape(TOKENS, HIDDEN)
    dw_down = mixed_dot(hidden_b.T, cot_mlp)
    d_pre = gelu_pull(mixed_dot(cot_mlp, w_down.T))[0].astype(jnp.bfloat16)
    dw_up = mixed_dot(u_mlp.T, d_pre)
    dy_one = dy_one + rms_back(y_one, mixed_dot(d_pre, w_up.T).reshape(STATE_SHAPE))
    u_att = rms_norm(x_two).astype(jnp.bfloat16).reshape(TOKENS, HIDDEN)
    qkv_seqs = mixed_dot(u_att, w_qkv_flat).astype(jnp.bfloat16).reshape(SEQ_COUNT, SEQ_LEN, N_HEADS, 3, HEAD_DIM).transpose(0, 3, 2, 1, 4)
    context = lax.map(attn_forward, qkv_seqs)
    context_flat = context.transpose(0, 2, 1, 3).reshape(TOKENS, HIDDEN)
    x_one = y_one - mixed_dot(context_flat, w_out_flat).reshape(STATE_SHAPE)
    cot_att = dy_one.astype(jnp.bfloat16).reshape(TOKENS, HIDDEN)
    dw_out = mixed_dot(context_flat.T, cot_att)
    d_context = mixed_dot(cot_att, w_out_flat.T).astype(jnp.bfloat16).reshape(SEQ_COUNT, SEQ_LEN, N_HEADS, HEAD_DIM).transpose(0, 2, 1, 3)
    d_qkv = lax.map(attn_backward, (qkv_seqs, d_context))
    d_qkv_flat = d_qkv.transpose(0, 3, 2, 1, 4).reshape(TOKENS, 3 * HIDDEN)
    dw_qkv = mixed_dot(u_att.T, d_qkv_flat)
    dx_two = dy_two + rms_back(x_two, mixed_dot(d_qkv_flat, w_qkv_flat.T).reshape(STATE_SHAPE))
    grads = (dw_qkv.reshape(HIDDEN, N_HEADS, 3, HEAD_DIM), dw_out.reshape(N_HEADS, HEAD_DIM, HIDDEN), dw_up, dw_down)
    return (x_one, x_two, dy_one, dx_two), grads


def reference(y_one, y_two, dy_one, dy_two, w_qkv, w_out, w_up, w_down):
    final_state, grad_stack = lax.scan(block_backward, (y_one, y_two, dy_one, dy_two), (w_qkv, w_out, w_up, w_down), reverse=True)
    x_one, x_two, dx_one, dx_two = final_state
    dw_qkv, dw_out, dw_up, dw_down = grad_stack
    return (x_one, x_two, dx_one, dx_two, dw_qkv, dw_out, dw_up, dw_down)
```

```python
import functools

import jax
import jax.numpy as jnp
from jax import lax
from jax.experimental import pallas as pl
from jax.experimental.pallas import tpu as pltpu
from jax.sharding import PartitionSpec as P

RMS_EPS = 1e-6
f32 = jnp.float32
bf16 = jnp.bfloat16

OWN, T, W, O, PC, TP, WP, OP = range(8)
XOR = (0, 6, 2, 4, 1, 7, 3, 5)
CORE, NEAR_T, NEAR_W = 1, 6, 2
AG_SEMS = 9
RS_SEMS = 10


def peer(mask):
    me = lax.axis_index("tp")
    out = me
    for bit in (1, 2, 4):
        if mask & bit:
            out = out + bit - 2 * bit * (lax.rem(out, 2 * bit) // bit)
    return {"tp": out}


def enter(masks):
    barrier = pltpu.get_barrier_semaphore()
    for mask in masks:
        pl.semaphore_signal(barrier, inc=1, device_id=peer(mask), device_id_type=pl.DeviceIdType.MESH)
    pl.semaphore_wait(barrier, len(masks))


def remote(src, dst, send, recv, index, mask):
    return pltpu.make_async_remote_copy(
        src_ref=src, dst_ref=dst, send_sem=send.at[index], recv_sem=recv.at[index],
        device_id=peer(mask), device_id_type=pl.DeviceIdType.MESH)


class Gather:
    def __init__(self, own, buf, send, recv):
        rows = own.shape[0]
        half = rows // 2

        def at(block, lo=0, size=rows):
            return buf.at[pl.ds(block * rows + lo, size)]

        self.own, self.buf, self.rows = own, buf, rows
        self.t = remote(own, at(T), send, recv, 0, NEAR_T)
        self.w = remote(own, at(W), send, recv, 1, NEAR_W)
        self.p = remote(own, at(PC), send, recv, 2, CORE)
        self.oa = remote(at(W, 0, half), at(O, 0, half), send, recv, 3, NEAR_T)
        self.ob = remote(at(T, half, half), at(O, half, half), send, recv, 4, NEAR_W)
        self.tp = remote(at(T), at(TP), send, recv, 5, CORE)
        self.wp = remote(at(W), at(WP), send, recv, 6, CORE)
        self.opa = remote(at(O, 0, half), at(OP, 0, half), send, recv, 7, CORE)
        self.opb = remote(at(O, half, half), at(OP, half, half), send, recv, 8, CORE)

    def start(self):
        self.t.start()
        self.w.start()
        self.p.start()

    def forward(self):
        self.t.wait_recv()
        self.ob.start()
        self.tp.start()
        self.w.wait_recv()
        self.oa.start()
        self.wp.start()

    def finish(self):
        self.oa.wait_recv()
        self.opa.start()
        self.ob.wait_recv()
        self.opb.start()

    def drain(self):
        for copy in (self.t, self.w, self.p, self.oa, self.ob, self.tp, self.wp, self.opa, self.opb):
            copy.wait_send()


class Scatter:
    def __init__(self, part, bufs, send, recv):
        self.part = part
        self.snd, self.kept, self.in_o, self.in_w, self.in_t = bufs
        rows = self.in_o.shape[0]
        half = rows // 2
        lo, hi = pl.ds(0, half), pl.ds(half, half)
        self.lo, self.hi = lo, hi
        self.d2d = [remote(self.snd.at[i % 2], self.kept.at[block], send, recv, i, CORE)
                    for i, block in enumerate((O, W, T, OWN))]
        self.oa = remote(self.kept.at[O, lo], self.in_o.at[lo], send, recv, 4, NEAR_T)
        self.ob = remote(self.kept.at[O, hi], self.in_o.at[hi], send, recv, 5, NEAR_W)
        self.w_hi = remote(self.kept.at[W, hi], self.in_w.at[hi], send, recv, 6, NEAR_W)
        self.t_lo = remote(self.kept.at[T, lo], self.in_t.at[lo], send, recv, 7, NEAR_T)
        self.w_lo = remote(self.kept.at[W, lo], self.in_w.at[lo], send, recv, 8, NEAR_W)
        self.t_hi = remote(self.kept.at[T, hi], self.in_t.at[hi], send, recv, 9, NEAR_T)

    def add(self, block):
        self.part(block, self.kept.at[block], True)

    def begin(self):
        for i, block in enumerate((OP, WP, TP, PC)):
            if i >= 2:
                self.d2d[i - 2].wait_send()
            self.part(block, self.snd.at[i % 2], False)
            self.d2d[i].start()
        self.d2d[0].wait_recv()
        self.add(O)
        self.oa.start()
        self.ob.start()
        self.d2d[1].wait_recv()
        self.add(W)
        self.w_hi.start()
        self.d2d[2].wait_recv()
        self.add(T)
        self.t_lo.start()
        self.d2d[3].wait_recv()
        self.add(OWN)

    def middle(self):
        self.oa.wait_recv()
        self.kept[W, self.lo] = self.kept[W, self.lo] + self.in_o[self.lo]
        self.w_lo.start()
        self.ob.wait_recv()
        self.kept[T, self.hi] = self.kept[T, self.hi] + self.in_o[self.hi]
        self.t_hi.start()

    def end(self, out):
        for copy in (self.w_hi, self.t_lo, self.w_lo, self.t_hi):
            copy.wait_recv()
        out[...] = self.kept[OWN] + self.in_w[...] + self.in_t[...]

    def drain(self):
        for copy in (self.d2d[2], self.d2d[3], self.oa, self.ob, self.w_hi, self.t_lo, self.w_lo, self.t_hi):
            copy.wait_send()


def dot(left, right, dims):
    return lax.dot_general(left, right, (dims, ((), ())), preferred_element_type=f32)


NN, NT, TN = ((1,), (0,)), ((1,), (1,)), ((0,), (0,))


def tiles(total, size, body):
    def step(i, carry):
        body(pl.ds(pl.multiple_of(i * size, size), size))
        return carry
    lax.fori_loop(0, total // size, step, 0)


def mlp_kernel(u_ref, c_ref, w1, w2, g_ref, du_ref, dw1, dw2, u_all, c_all, act, hid, dpre,
               g_snd, g_kept, g_o, g_w, g_t, d_snd, d_kept, d_o, d_w, d_t,
               us, ur, cs, cr, gs, gr, ds, dr):
    enter((CORE, NEAR_T, NEAR_W))
    rows, hidden = u_ref.shape
    cols = w1.shape[1]
    tile = 128
    gu = Gather(u_ref, u_all, us, ur)
    gc = Gather(c_ref, c_all, cs, cr)

    def block_rows(block):
        return pl.ds(block * rows, rows)

    def up(block):
        here = block_rows(block)
        src = u_ref if block == OWN else u_all.at[here]

        def body(col):
            a = dot(src[...], w1[:, col], NN)
            hid[here, col] = jax.nn.gelu(a, approximate=True).astype(bf16)
            act[here, col] = a
        tiles(cols, tile, body)

    def down(block):
        here = block_rows(block)
        src = c_ref if block == OWN else c_all.at[here]

        def body(col):
            dh = dot(src[...], w2[col, :], NT)
            _, pull = jax.vjp(lambda a: jax.nn.gelu(a, approximate=True), act[here, col])
            dpre[here, col] = pull(dh)[0].astype(bf16)
        tiles(cols, tile, body)

    def part_of(lhs, rhs, transposed):
        def part(block, out, accumulate):
            here = block_rows(block)

            def body(col):
                value = dot(lhs[here], rhs[col, :], NT) if transposed else dot(lhs[here], rhs[:, col], NN)
                out[:, col] = out[:, col] + value if accumulate else value
            tiles(hidden, 256, body)
        return part

    rs_g = Scatter(part_of(hid, w2, False), (g_snd, g_kept, g_o, g_w, g_t), gs, gr)
    rs_d = Scatter(part_of(dpre, w1, True), (d_snd, d_kept, d_o, d_w, d_t), ds, dr)

    gu.start()
    u_all[block_rows(OWN)] = u_ref[...]
    up(OWN)
    gu.p.wait_recv()
    up(PC)
    gu.forward()
    gc.start()
    c_all[block_rows(OWN)] = c_ref[...]
    up(T)
    up(W)
    gu.tp.wait_recv()
    up(TP)
    gu.wp.wait_recv()
    up(WP)
    gu.finish()
    up(O)
    gu.opa.wait_recv()
    gu.opb.wait_recv()
    up(OP)
    down(OWN)
    gc.p.wait_recv()
    down(PC)
    gc.forward()
    rs_g.begin()
    down(T)
    down(W)
    gc.tp.wait_recv()
    down(TP)
    gc.wp.wait_recv()
    down(WP)
    gc.finish()
    rs_g.middle()
    down(O)
    gc.opa.wait_recv()
    gc.opb.wait_recv()
    down(OP)
    rs_d.begin()

    def body1(col):
        dw1[:, col] = dot(u_all[...], dpre[:, col], TN)

    def body2(col):
        dw2[col, :] = dot(hid[:, col], c_all[...], TN)
    tiles(cols, tile, body2)
    rs_d.middle()
    rs_g.end(g_ref)
    tiles(cols, tile, body1)
    rs_d.end(du_ref)
    for item in (gu, gc, rs_g, rs_d):
        item.drain()


def attn_kernel(scale, u_ref, c_ref, wq, wk, wv, wo, f_ref, du_ref, dwq, dwk, dwv, dwo,
                u_all, c_all, wo_all, q_all, k_all, v_all, dctx, ctx, ctx_in, prob,
                d_snd, d_kept, d_o, d_w, d_t, us, ur, cs, cr, ws, wr, xs, xr, ds, dr):
    enter(XOR[1:])
    rows, hidden = u_ref.shape
    width = wq.shape[1]
    head = width // 2
    pos = 32
    n_seq = rows // pos
    gu = Gather(u_ref, u_all, us, ur)
    gc = Gather(c_ref, c_all, cs, cr)
    gw = Gather(wo, wo_all, ws, wr)
    lanes = lax.broadcasted_iota(jnp.int32, (1, width), 1)
    masks = [(lanes < head), (lanes >= head)]

    def block_rows(block):
        return pl.ds(block * rows, rows)

    def pick(value, n):
        return jnp.where(masks[n], value, jnp.zeros_like(value))

    def qkv(block):
        here = block_rows(block)
        src = u_ref if block == OWN else u_all.at[here]
        value = src[...]
        for weight, out in ((wq, q_all), (wk, k_all), (wv, v_all)):
            out[here] = dot(value, weight[...], NN).astype(bf16)

    def d_ctx(block):
        here = block_rows(block)
        src = c_ref if block == OWN else c_all.at[here]
        dctx[here] = dot(src[...], wo[...], NT).astype(bf16)

    def seq_get(ref, seq):
        return jnp.concatenate([ref[pl.ds(pl.multiple_of(b * rows + seq * pos, pos), pos)] for b in range(8)], axis=0)

    def seq_put(ref, seq, value):
        for b in range(8):
            ref[pl.ds(pl.multiple_of(b * rows + seq * pos, pos), pos)] = value[b * pos:(b + 1) * pos]

    def forward(seq, carry):
        q, k, v = seq_get(q_all, seq), seq_get(k_all, seq), seq_get(v_all, seq)
        total = None
        for n in range(2):
            scores = dot(pick(q, n), k, NT) * scale
            expd = jnp.exp(scores - jnp.max(scores, axis=-1, keepdims=True))
            p = expd / jnp.sum(expd, axis=-1, keepdims=True)
            prob[2 * seq + n] = p
            out = dot(p.astype(bf16), pick(v, n), NN)
            total = out if total is None else total + out
        seq_put(ctx, seq, total.astype(bf16))
        return carry

    def backward(seq, carry):
        q, k, v, do = seq_get(q_all, seq), seq_get(k_all, seq), seq_get(v_all, seq), seq_get(dctx, seq)
        sums = [None, None, None]
        for n in range(2):
            p = prob[2 * seq + n]
            dp = dot(pick(do, n), v, NT)
            terms = [None, None, dot(p.astype(bf16), pick(do, n), TN)]
            dsc = (p * (dp - jnp.sum(dp * p, axis=-1, keepdims=True)) * scale).astype(bf16)
            terms[0] = dot(dsc, pick(k, n), NN)
            terms[1] = dot(dsc, pick(q, n), TN)
            sums = [b if a is None else a + b for a, b in zip(sums, terms)]
        for ref, value in zip((q_all, k_all, v_all), sums):
            seq_put(ref, seq, value.astype(bf16))
        return carry

    def part(block, out, accumulate):
        here = block_rows(block)

        def body(col):
            value = dot(q_all[here], wq[col, :], NT) + dot(k_all[here], wk[col, :], NT) + dot(v_all[here], wv[col, :], NT)
            out[:, col] = out[:, col] + value if accumulate else value
        tiles(hidden, 256, body)

    rs_d = Scatter(part, (d_snd, d_kept, d_o, d_w, d_t), ds, dr)
    out_rows = wo.shape[0]
    shares = [remote(ctx.at[block_rows(b)], ctx_in.at[b], xs, xr, b - 1, XOR[b]) for b in range(1, 8)]

    gu.start()
    u_all[block_rows(OWN)] = u_ref[...]
    qkv(OWN)
    gu.p.wait_recv()
    qkv(PC)
    gu.forward()
    gc.start()
    c_all[block_rows(OWN)] = c_ref[...]
    wo_all[pl.ds(0, out_rows)] = wo[...]
    qkv(T)
    qkv(W)
    gu.tp.wait_recv()
    qkv(TP)
    gu.wp.wait_recv()
    qkv(WP)
    gu.finish()
    qkv(O)
    gu.opa.wait_recv()
    gu.opb.wait_recv()
    qkv(OP)
    lax.fori_loop(0, n_seq, forward, 0)
    gc.forward()
    for copy in shares:
        copy.start()
    gw.start()
    d_ctx(OWN)
    gc.p.wait_recv()
    d_ctx(PC)
    d_ctx(T)
    d_ctx(W)
    gc.tp.wait_recv()
    d_ctx(TP)
    gc.wp.wait_recv()
    d_ctx(WP)
    gc.finish()
    d_ctx(O)
    gc.opa.wait_recv()
    gc.opb.wait_recv()
    d_ctx(OP)
    lax.fori_loop(0, n_seq, backward, 0)
    rs_d.begin()
    gw.forward()
    dwo[...] = dot(ctx[...], c_all[...], TN)
    gw.finish()
    rs_d.middle()
    dwq[...] = dot(u_all[...], q_all[...], TN)
    dwk[...] = dot(u_all[...], k_all[...], TN)
    dwv[...] = dot(u_all[...], v_all[...], TN)
    for copy in shares:
        copy.wait_recv()
    for copy in (gw.p, gw.tp, gw.wp, gw.opa, gw.opb):
        copy.wait_recv()

    def f_body(col):
        total = dot(ctx[block_rows(OWN)], wo_all[pl.ds(0, out_rows), col], NN)
        for b in range(1, 8):
            total = total + dot(ctx_in[b], wo_all[pl.ds(b * out_rows, out_rows), col], NN)
        f_ref[:, col] = total
    tiles(hidden, 256, f_body)
    rs_d.end(du_ref)
    for item in (gu, gc, gw, rs_d):
        item.drain()
    for copy in shares:
        copy.wait_send()


def vmem(shape, dtype):
    return pltpu.VMEM(shape, dtype)


def scatter_scratch(rows, hidden):
    return [vmem((2, rows, hidden), f32), vmem((4, rows, hidden), f32)] + [vmem((rows, hidden), f32)] * 3


def sems(count):
    return [pltpu.SemaphoreType.DMA((count,))] * 2


def call(kernel, outs, scratch, collective_id, name, flops, *args):
    spec = pl.BlockSpec(memory_space=pltpu.VMEM)
    return pl.pallas_call(
        kernel,
        out_shape=[jax.ShapeDtypeStruct(shape, f32) for shape in outs],
        in_specs=[spec] * len(args),
        out_specs=[spec] * len(outs),
        scratch_shapes=scratch,
        name=name,
        cost_estimate=pl.CostEstimate(flops=flops, bytes_accessed=10 ** 7, transcendentals=0),
        compiler_params=pltpu.CompilerParams(
            collective_id=collective_id, has_side_effects=True, vmem_limit_bytes=67043328),
    )(*args)


def mlp_block(u, c, w1, w2):
    rows, hidden = u.shape
    cols = w1.shape[1]
    total = 8 * rows
    scratch = [vmem((total, hidden), bf16)] * 2 + [vmem((total, cols), f32)] + [vmem((total, cols), bf16)] * 2
    scratch += scatter_scratch(rows, hidden) * 2 + sems(AG_SEMS) * 2 + sems(RS_SEMS) * 2
    outs = [(rows, hidden)] * 2 + [(hidden, cols), (cols, hidden)]
    return call(mlp_kernel, outs, scratch, 0, "mlp_block", 12 * total * hidden * cols, u, c, w1, w2)


def attn_block(scale, u, c, wq, wk, wv, wo):
    rows, hidden = u.shape
    width = wq.shape[1]
    total = 8 * rows
    scratch = [vmem((total, hidden), bf16)] * 2 + [vmem((8 * wo.shape[0], hidden), bf16)]
    scratch += [vmem((total, width), bf16)] * 5 + [vmem((8, rows, width), bf16), vmem((16, 256, 256), f32)]
    scratch += scatter_scratch(rows, hidden) + sems(AG_SEMS) * 3 + sems(7) + sems(RS_SEMS)
    outs = [(rows, hidden)] * 2 + [(hidden, width)] * 3 + [(width, hidden)]
    kernel = functools.partial(attn_kernel, scale)
    return call(kernel, outs, scratch, 1, "attn_block", 24 * total * hidden * width, u, c, wq, wk, wv, wo)


def inv_rms_of(tensor):
    return lax.rsqrt(jnp.mean(tensor * tensor, axis=-1, keepdims=True) + RMS_EPS)


def rms_norm(tensor):
    return tensor * inv_rms_of(tensor)


def rms_back(tensor, grad_in):
    inv_rms = inv_rms_of(tensor)
    return inv_rms * grad_in - tensor * (inv_rms * inv_rms * inv_rms) * jnp.mean(grad_in * tensor, axis=-1, keepdims=True)


def local_backward(y_one, y_two, dy_one, dy_two, w_qkv, w_out, w_up, w_down):
    n_layers, hidden, heads, _, head_dim = w_qkv.shape
    width = heads * head_dim
    state_shape = y_one.shape
    y_one, y_two, dy_one, dy_two = [x.reshape(-1, hidden) for x in (y_one, y_two, dy_one, dy_two)]
    grads_qkv, grads_out, grads_up, grads_down = [], [], [], []
    for layer in reversed(range(n_layers)):
        wq, wk, wv = [w_qkv[layer, :, :, j].reshape(hidden, width) for j in range(3)]
        wo = w_out[layer].reshape(width, hidden)
        g_out, du_mlp, dw_up, dw_down = mlp_block(
            rms_norm(y_one).astype(bf16), dy_two.astype(bf16), w_up[layer], w_down[layer])
        x_two = y_two - g_out
        dy_one = dy_one + rms_back(y_one, du_mlp)
        f_out, du_att, dwq, dwk, dwv, dwo = attn_block(
            head_dim ** -0.5, rms_norm(x_two).astype(bf16), dy_one.astype(bf16), wq, wk, wv, wo)
        x_one = y_one - f_out
        dx_two = dy_two + rms_back(x_two, du_att)
        grads_up.append(dw_up)
        grads_down.append(dw_down)
        grads_out.append(dwo.reshape(heads, head_dim, hidden))
        grads_qkv.append(jnp.stack([g.reshape(hidden, heads, head_dim) for g in (dwq, dwk, dwv)], axis=2))
        y_one, y_two, dy_two = x_one, x_two, dx_two
    state = [x.reshape(state_shape) for x in (y_one, y_two, dy_one, dy_two)]
    return (*state, jnp.stack(grads_qkv[::-1]), jnp.stack(grads_out[::-1]), jnp.stack(grads_up[::-1]), jnp.stack(grads_down[::-1]))


def solution(mesh):
    state_spec = P("dp", "tp", None)
    in_specs = (state_spec, state_spec, state_spec, state_spec, P(None, None, "tp", None, None), P(None, "tp", None, None), P(None, None, "tp"), P(None, "tp", None))
    out_specs = (state_spec, state_spec, state_spec, state_spec, P("dp", None, "tp", None, None), P("dp", "tp", None, None), P("dp", None, "tp"), P("dp", "tp", None))
    return jax.shard_map(local_backward, mesh=mesh, in_specs=in_specs, out_specs=out_specs, check_vma=False)
```

```python
import functools

import jax
import jax.numpy as jnp
from jax import lax
from jax.experimental import pallas as pl
from jax.experimental.pallas import tpu as pltpu
from jax.sharding import PartitionSpec as P

RMS_EPS = 1e-6
f32 = jnp.float32
bf16 = jnp.bfloat16

OWN, T, W, O, PC, TP, WP, OP = range(8)
XOR = (0, 6, 2, 4, 1, 7, 3, 5)
CORE, NEAR_T, NEAR_W = 1, 6, 2
AG_SEMS = 9
RS_SEMS = 10
NN, NT, TN = ((1,), (0,)), ((1,), (1,)), ((0,), (0,))


def peer(mask):
    out = lax.axis_index("tp")
    for bit in (1, 2, 4):
        if mask & bit:
            out = out + bit - 2 * bit * (lax.rem(out, 2 * bit) // bit)
    return {"tp": out}


def enter(masks):
    barrier = pltpu.get_barrier_semaphore()
    for mask in masks:
        pl.semaphore_signal(barrier, inc=1, device_id=peer(mask), device_id_type=pl.DeviceIdType.MESH)
    pl.semaphore_wait(barrier, len(masks))


def remote(src, dst, send, recv, index, mask):
    return pltpu.make_async_remote_copy(
        src_ref=src, dst_ref=dst, send_sem=send.at[index], recv_sem=recv.at[index],
        device_id=peer(mask), device_id_type=pl.DeviceIdType.MESH)


def dot(left, right, dims):
    return lax.dot_general(left, right, (dims, ((), ())), preferred_element_type=f32)


def loop(count, body):
    def step(i, carry):
        body(i)
        return carry
    lax.fori_loop(0, count, step, 0)


def tiles(total, size, body):
    loop(total // size, lambda i: body(pl.ds(pl.multiple_of(i * size, size), size)))


class Gather:
    def __init__(self, buf, send, recv):
        rows = buf.shape[0] // 8
        half = rows // 2

        def at(block, lo=0, size=rows):
            return buf.at[pl.ds(block * rows + lo, size)]

        self.t = remote(at(OWN), at(T), send, recv, 0, NEAR_T)
        self.w = remote(at(OWN), at(W), send, recv, 1, NEAR_W)
        self.p = remote(at(OWN), at(PC), send, recv, 2, CORE)
        self.oa = remote(at(W, 0, half), at(O, 0, half), send, recv, 3, NEAR_T)
        self.ob = remote(at(T, half, half), at(O, half, half), send, recv, 4, NEAR_W)
        self.tp = remote(at(T), at(TP), send, recv, 5, CORE)
        self.wp = remote(at(W), at(WP), send, recv, 6, CORE)
        self.opa = remote(at(O, 0, half), at(OP, 0, half), send, recv, 7, CORE)
        self.opb = remote(at(O, half, half), at(OP, half, half), send, recv, 8, CORE)

    def start(self):
        self.t.start()
        self.w.start()
        self.p.start()

    def forward(self):
        self.t.wait_recv()
        self.ob.start()
        self.tp.start()
        self.w.wait_recv()
        self.oa.start()
        self.wp.start()

    def finish(self):
        self.oa.wait_recv()
        self.opa.start()
        self.ob.wait_recv()
        self.opb.start()

    def last(self):
        self.opa.wait_recv()
        self.opb.wait_recv()

    def drain(self):
        for copy in (self.t, self.w, self.p, self.oa, self.ob, self.tp, self.wp, self.opa, self.opb):
            copy.wait_send()

    def each_block(self, compute, after_forward=None, forwarded=False):
        def body(step):
            if not forwarded:
                @pl.when(step == 2)
                def _():
                    self.forward()
                    if after_forward is not None:
                        after_forward()
            for when, act in ((1, self.p.wait_recv), (3, self.tp.wait_recv), (5, self.wp.wait_recv), (6, self.finish), (7, self.last)):
                pl.when(step == when)(act)
            compute(step // 2 + 4 * lax.rem(step, 2))
        loop(8, body)


class Scatter:
    def __init__(self, part, bufs, send, recv):
        self.part, self.send, self.recv = part, send, recv
        self.snd, self.kept, self.in_o, self.in_w, self.in_t = bufs
        half = self.in_o.shape[0] // 2
        lo, hi = pl.ds(0, half), pl.ds(half, half)
        self.lo, self.hi = lo, hi
        self.oa = remote(self.kept.at[O, lo], self.in_o.at[lo], send, recv, 4, NEAR_T)
        self.ob = remote(self.kept.at[O, hi], self.in_o.at[hi], send, recv, 5, NEAR_W)
        self.w_hi = remote(self.kept.at[W, hi], self.in_w.at[hi], send, recv, 6, NEAR_W)
        self.t_lo = remote(self.kept.at[T, lo], self.in_t.at[lo], send, recv, 7, NEAR_T)
        self.w_lo = remote(self.kept.at[W, lo], self.in_w.at[lo], send, recv, 8, NEAR_W)
        self.t_hi = remote(self.kept.at[T, hi], self.in_t.at[hi], send, recv, 9, NEAR_T)

    def d2d(self, i):
        return remote(self.snd.at[lax.rem(i, 2)], self.kept.at[3 - i], self.send, self.recv, i, CORE)

    def begin(self):
        def theirs(i):
            @pl.when(i >= 2)
            def _():
                self.d2d(i - 2).wait_send()
            self.part(7 - i, self.snd.at[lax.rem(i, 2)], False)
            self.d2d(i).start()
        loop(4, theirs)

        def mine(i):
            self.d2d(i).wait_recv()
            self.part(3 - i, self.kept.at[3 - i], True)

            @pl.when(i == 0)
            def _():
                self.oa.start()
                self.ob.start()
            pl.when(i == 1)(self.w_hi.start)
            pl.when(i == 2)(self.t_lo.start)
        loop(4, mine)

    def middle(self):
        self.oa.wait_recv()
        self.kept[W, self.lo] = self.kept[W, self.lo] + self.in_o[self.lo]
        self.w_lo.start()
        self.ob.wait_recv()
        self.kept[T, self.hi] = self.kept[T, self.hi] + self.in_o[self.hi]
        self.t_hi.start()

    def end(self):
        for copy in (self.w_hi, self.t_lo, self.w_lo, self.t_hi):
            copy.wait_recv()

    def result(self, here):
        return self.kept[OWN, here] + self.in_w[here] + self.in_t[here]

    def drain(self, slots=True):
        if slots:
            self.free_slots()
        for copy in (self.oa, self.ob, self.w_hi, self.t_lo, self.w_lo, self.t_hi):
            copy.wait_send()

    def free_slots(self):
        self.d2d(2).wait_send()
        self.d2d(3).wait_send()


ROW_TILE = 32


def inv_rms_of(tensor):
    return lax.rsqrt(jnp.mean(tensor * tensor, axis=-1, keepdims=True) + RMS_EPS)


def rms_norm(tensor):
    return tensor * inv_rms_of(tensor)


def rms_back(tensor, grad_in):
    inv_rms = inv_rms_of(tensor)
    return inv_rms * grad_in - tensor * (inv_rms * inv_rms * inv_rms) * jnp.mean(grad_in * tensor, axis=-1, keepdims=True)


def gelu_tanh(tensor):
    return jax.nn.gelu(tensor, approximate=True)


def mlp_kernel(layer, y1, dy2, y2_hbm, dy1_hbm, w1_hbm, w2_hbm, x2_out, dy1_out, dw1_hbm, dw2_hbm,
               w1, w2, u_all, c_all, act, hid, dpre, tmp, dw1, dw2,
               g_snd, g_kept, g_o, g_w, g_t, d_snd, d_kept, d_o, d_w, d_t,
               us, ur, cs, cr, gs, gr, ds, dr, local):
    rows, hidden = y1.shape
    cols = w1.shape[1]
    get_w1 = pltpu.make_async_copy(w1_hbm.at[layer], w1, local.at[0])
    get_w2 = pltpu.make_async_copy(w2_hbm.at[layer], w2, local.at[1])
    get_w1.start()
    get_w2.start()
    gu = Gather(u_all, us, ur)
    gc = Gather(c_all, cs, cr)

    def block_rows(block):
        return pl.ds(pl.multiple_of(block * rows, rows), rows)

    def norm_in(here):
        u_all[here] = rms_norm(y1[here]).astype(bf16)
    tiles(rows, ROW_TILE, norm_in)
    enter((CORE, NEAR_T, NEAR_W))
    gu.start()

    def cast_in(here):
        c_all[here] = dy2[here].astype(bf16)
    tiles(rows, ROW_TILE, cast_in)
    get_w1.wait()
    get_w2.wait()

    def up(block):
        here = block_rows(block)
        act[here] = dot(u_all[here], w1[...], NN)

        def body(i):
            some = pl.ds(pl.multiple_of(block * rows + i * ROW_TILE, ROW_TILE), ROW_TILE)
            hid[some] = gelu_tanh(act[some]).astype(bf16)
        loop(rows // ROW_TILE, body)

    def down(block):
        tmp[...] = dot(c_all[block_rows(block)], w2[...], NT)

        def body(i):
            some = pl.ds(pl.multiple_of(block * rows + i * ROW_TILE, ROW_TILE), ROW_TILE)
            _, pull = jax.vjp(gelu_tanh, act[some])
            dpre[some] = pull(tmp[pl.ds(pl.multiple_of(i * ROW_TILE, ROW_TILE), ROW_TILE)])[0].astype(bf16)
        loop(rows // ROW_TILE, body)

    def part_of(lhs, rhs, transposed):
        def part(block, out, accumulate):
            here = block_rows(block)

            def body(col):
                value = dot(lhs[here], rhs[col, :], NT) if transposed else dot(lhs[here], rhs[:, col], NN)
                out[:, col] = out[:, col] + value if accumulate else value
            tiles(hidden, 256, body)
        return part

    rs_g = Scatter(part_of(hid, w2, False), (g_snd, g_kept, g_o, g_w, g_t), gs, gr)
    rs_d = Scatter(part_of(dpre, w1, True), (d_snd, d_kept, d_o, d_w, d_t), ds, dr)

    gu.each_block(up, gc.start)

    def between():
        rs_g.begin()
    gc.each_block(down, between)
    rs_g.middle()
    rs_d.begin()
    rs_g.free_slots()
    get_y2 = pltpu.make_async_copy(y2_hbm, g_snd.at[0], local.at[2])
    get_dy1 = pltpu.make_async_copy(dy1_hbm, g_snd.at[1], local.at[3])
    get_y2.start()
    get_dy1.start()

    def body2(col):
        dw2[col, :] = dot(hid[:, col], c_all[...], TN)
    tiles(cols, 128, body2)
    put_dw2 = pltpu.make_async_copy(dw2, dw2_hbm, local.at[0])
    put_dw2.start()
    rs_d.middle()
    rs_g.end()
    get_y2.wait()

    def x2_body(here):
        x2_out[here] = g_snd[0, here] - rs_g.result(here)
    tiles(rows, ROW_TILE, x2_body)

    def body1(col):
        dw1[col, :] = dot(u_all[:, col], dpre[...], TN)
    tiles(hidden, 256, body1)
    put_dw1 = pltpu.make_async_copy(dw1, dw1_hbm, local.at[1])
    put_dw1.start()
    get_dy1.wait()
    rs_d.end()

    def dy1_body(here):
        dy1_out[here] = g_snd[1, here] + rms_back(y1[here], rs_d.result(here))
    tiles(rows, ROW_TILE, dy1_body)
    gu.drain()
    gc.drain()
    rs_g.drain(False)
    rs_d.drain()
    put_dw2.wait()
    put_dw1.wait()


def attn_kernel(layer, scale, x2, dy1, y1, dy2, wqkv_hbm, wo_hbm, x1_out, dx2_out, dwqkv, dwo,
                wq, wk, wv, wo_all, u_all, c_all, q_all, k_all, v_all, dctx, ctx, ctx_in, prob,
                a_snd, a_kept, a_o, a_w, a_t, b_snd, b_kept, b_o, b_w, b_t,
                us, ur, cs, cr, ws, wr, xs, xr, as_, ar, bs, br, local):
    rows, hidden = x2.shape
    width = wq.shape[0]
    head = width // 2
    pos = 32
    n_seq = rows // pos
    gets = []
    for n in range(2):
        for j, ref in enumerate((wq, wk, wv)):
            gets.append(pltpu.make_async_copy(wqkv_hbm.at[layer, n, j], ref.at[pl.ds(n * head, head)], local.at[len(gets)]))
    gets.append(pltpu.make_async_copy(wo_hbm.at[layer], wo_all.at[pl.ds(0, width)], local.at[len(gets)]))
    for copy in gets:
        copy.start()
    gu = Gather(u_all, us, ur)
    gc = Gather(c_all, cs, cr)
    gw = Gather(wo_all, ws, wr)
    lanes = lax.broadcasted_iota(jnp.int32, (1, width), 1)
    masks = [(lanes < head), (lanes >= head)]

    def norm_in(here):
        u_all[here] = rms_norm(x2[here]).astype(bf16)
    tiles(rows, ROW_TILE, norm_in)
    enter(XOR[1:])
    gu.start()

    def cast_in(here):
        c_all[here] = dy1[here].astype(bf16)
    tiles(rows, ROW_TILE, cast_in)
    for copy in gets:
        copy.wait()

    def block_rows(block):
        return pl.ds(pl.multiple_of(block * rows, rows), rows)

    def pick(value, n):
        return jnp.where(masks[n], value, jnp.zeros_like(value))

    def qkv(block):
        here = block_rows(block)
        value = u_all[here]
        for weight, out in ((wq, q_all), (wk, k_all), (wv, v_all)):
            out[here] = dot(value, weight[...], NT).astype(bf16)

    def d_ctx(block):
        here = block_rows(block)
        dctx[here] = dot(c_all[here], wo_all[pl.ds(0, width)], NT).astype(bf16)

    def seq_get(ref, seq):
        return jnp.concatenate([ref[pl.ds(pl.multiple_of(b * rows + seq * pos, pos), pos)] for b in range(8)], axis=0)

    def seq_put(ref, seq, value):
        for b in range(8):
            ref[pl.ds(pl.multiple_of(b * rows + seq * pos, pos), pos)] = value[b * pos:(b + 1) * pos]

    def forward(seq):
        q, k, v = seq_get(q_all, seq), seq_get(k_all, seq), seq_get(v_all, seq)
        total = None
        for n in range(2):
            scores = dot(pick(q, n), k, NT) * scale
            expd = jnp.exp(scores - jnp.max(scores, axis=-1, keepdims=True))
            p = expd / jnp.sum(expd, axis=-1, keepdims=True)
            prob[2 * seq + n] = p
            out = dot(p.astype(bf16), pick(v, n), NN)
            total = out if total is None else total + out
        seq_put(ctx, seq, total.astype(bf16))

    def backward(seq):
        q, k, v, do = seq_get(q_all, seq), seq_get(k_all, seq), seq_get(v_all, seq), seq_get(dctx, seq)
        sums = [None, None, None]
        for n in range(2):
            p = prob[2 * seq + n]
            dp = dot(pick(do, n), v, NT)
            d_value = dot(p.astype(bf16), pick(do, n), TN)
            dsc = (p * (dp - jnp.sum(dp * p, axis=-1, keepdims=True)) * scale).astype(bf16)
            terms = [dot(dsc, pick(k, n), NN), dot(dsc, pick(q, n), TN), d_value]
            sums = [b if a is None else a + b for a, b in zip(sums, terms)]
        for ref, value in zip((q_all, k_all, v_all), sums):
            seq_put(ref, seq, value.astype(bf16))

    half = rows // 2

    def part_of(chunk):
        def part(block, out, accumulate):
            here = pl.ds(pl.multiple_of(block * rows + chunk * half, half), half)

            def body(col):
                value = dot(q_all[here], wq[:, col], NN) + dot(k_all[here], wk[:, col], NN) + dot(v_all[here], wv[:, col], NN)
                out[:, col] = out[:, col] + value if accumulate else value
            tiles(hidden, 256, body)
        return part

    rs_a = Scatter(part_of(0), (a_snd, a_kept, a_o, a_w, a_t), as_, ar)
    rs_b = Scatter(part_of(1), (b_snd, b_kept, b_o, b_w, b_t), bs, br)
    shares = [remote(ctx.at[pl.ds(b * rows, rows)], ctx_in.at[b], xs, xr, b - 1, XOR[b]) for b in range(1, 8)]

    gu.each_block(qkv, gc.start)
    loop(n_seq // 2, forward)
    gc.forward()
    loop(n_seq // 2, lambda i: forward(i + n_seq // 2))
    for copy in shares:
        copy.start()
    gw.start()
    gc.each_block(d_ctx, forwarded=True)
    loop(n_seq // 2, backward)
    gw.forward()
    rs_a.begin()
    loop(n_seq // 2, lambda i: backward(i + n_seq // 2))
    rs_a.middle()
    rs_b.begin()
    dwo[...] = dot(ctx[...], c_all[...], TN)
    gw.finish()
    for i, ref in enumerate((q_all, k_all, v_all)):
        grad = dot(ref[...], u_all[...], TN)
        for n in range(2):
            dwqkv[n, i] = grad[n * head:(n + 1) * head]
    rs_b.middle()
    for copy in shares:
        copy.wait_recv()
    for copy in (gw.p, gw.tp, gw.wp):
        copy.wait_recv()
    gw.last()

    def f_body(col):
        total = dot(ctx[pl.ds(0, rows)], wo_all[pl.ds(0, width), col], NN)
        for b in range(1, 8):
            total = total + dot(ctx_in[b], wo_all[pl.ds(b * width, width), col], NN)
        x1_out[:, col] = y1[:, col] - total
    tiles(hidden, 256, f_body)
    for chunk, item in enumerate((rs_a, rs_b)):
        item.end()

        def dx_body(i):
            part_rows = pl.ds(pl.multiple_of(i * ROW_TILE, ROW_TILE), ROW_TILE)
            here = pl.ds(pl.multiple_of(chunk * half + i * ROW_TILE, ROW_TILE), ROW_TILE)
            dx2_out[here] = dy2[here] + rms_back(x2[here], item.result(part_rows))
        loop(half // ROW_TILE, dx_body)
    for item in (gu, gc, gw, rs_a, rs_b):
        item.drain()
    for copy in shares:
        copy.wait_send()


def vmem(shape, dtype):
    return pltpu.VMEM(shape, dtype)


def scatter_scratch(rows, hidden):
    return [vmem((2, rows, hidden), f32), vmem((4, rows, hidden), f32)] + [vmem((rows, hidden), f32)] * 3


def sems(count):
    return [pltpu.SemaphoreType.DMA((count,))] * 2


def call(kernel, outs, scratch, collective_id, name, flops, near, far):
    inside, outside = pl.BlockSpec(memory_space=pltpu.VMEM), pl.BlockSpec(memory_space=pl.ANY)
    return pl.pallas_call(
        kernel,
        out_shape=[jax.ShapeDtypeStruct(shape, f32) for shape, _ in outs],
        in_specs=[inside] * len(near) + [outside] * len(far),
        out_specs=[inside if kept else outside for _, kept in outs],
        scratch_shapes=scratch,
        name=name,
        cost_estimate=pl.CostEstimate(flops=flops, bytes_accessed=10 ** 7, transcendentals=0),
        compiler_params=pltpu.CompilerParams(
            collective_id=collective_id, has_side_effects=True, vmem_limit_bytes=67043328),
    )(*near, *far)


def mlp_block(layer, y1, dy2, y2, dy1, w1, w2):
    rows, hidden = y1.shape
    cols = w1.shape[2]
    total = 8 * rows
    scratch = [vmem((hidden, cols), bf16), vmem((cols, hidden), bf16)]
    scratch += [vmem((total, hidden), bf16)] * 2 + [vmem((total, cols), f32)] + [vmem((total, cols), bf16)] * 2
    scratch += [vmem((rows, cols), f32), vmem((hidden, cols), f32), vmem((cols, hidden), f32)]
    scratch += scatter_scratch(rows, hidden) * 2 + sems(AG_SEMS) * 2 + sems(RS_SEMS) * 2 + sems(4)[:1]
    outs = [((rows, hidden), True)] * 2 + [((hidden, cols), False), ((cols, hidden), False)]
    kernel = functools.partial(mlp_kernel, layer)
    return call(kernel, outs, scratch, 2 * layer, "mlp_block", 12 * total * hidden * cols, (y1, dy2), (y2, dy1, w1, w2))


def attn_block(layer, scale, x2, dy1, y1, dy2, wqkv, wo):
    rows, hidden = x2.shape
    _, heads, _, head, _ = wqkv.shape
    width = heads * head
    total = 8 * rows
    scratch = [vmem((width, hidden), bf16)] * 3 + [vmem((8 * width, hidden), bf16)] + [vmem((total, hidden), bf16)] * 2
    scratch += [vmem((total, width), bf16)] * 5 + [vmem((8, rows, width), bf16), vmem((16, 256, 256), f32)]
    scratch += scatter_scratch(rows // 2, hidden) * 2 + sems(AG_SEMS) * 3 + sems(7) + sems(RS_SEMS) * 2 + sems(7)[:1]
    outs = [((rows, hidden), True)] * 2 + [((heads, 3, head, hidden), True), ((width, hidden), True)]
    kernel = functools.partial(attn_kernel, layer, scale)
    return call(kernel, outs, scratch, 2 * layer + 1, "attn_block", 24 * total * hidden * width, (x2, dy1, y1, dy2), (wqkv, wo))


def local_backward(y_one, y_two, dy_one, dy_two, w_qkv, w_out, w_up, w_down):
    n_layers, hidden, heads, _, head_dim = w_qkv.shape
    state_shape = y_one.shape
    y_one, y_two, dy_one, dy_two = [x.reshape(-1, hidden) for x in (y_one, y_two, dy_one, dy_two)]
    w_qkv = w_qkv.transpose(0, 2, 3, 4, 1)
    w_out = w_out.reshape(n_layers, heads * head_dim, hidden)
    grads = []
    for layer in reversed(range(n_layers)):
        y_two, dy_one, dw_up, dw_down = mlp_block(layer, y_one, dy_two, y_two, dy_one, w_up, w_down)
        y_one, dy_two, dw_qkv, dw_out = attn_block(layer, head_dim ** -0.5, y_two, dy_one, y_one, dy_two, w_qkv, w_out)
        grads.append((dw_qkv, dw_out.reshape(heads, head_dim, hidden), dw_up, dw_down))
    d_qkv, d_out, d_up, d_down = [jnp.stack(g) for g in zip(*grads[::-1])]
    state = [x.reshape(state_shape) for x in (y_one, y_two, dy_one, dy_two)]
    return (*state, d_qkv.transpose(0, 4, 1, 2, 3), d_out, d_up, d_down)


def solution(mesh):
    state_spec = P("dp", "tp", None)
    in_specs = (state_spec, state_spec, state_spec, state_spec, P(None, None, "tp", None, None), P(None, "tp", None, None), P(None, None, "tp"), P(None, "tp", None))
    out_specs = (state_spec, state_spec, state_spec, state_spec, P("dp", None, "tp", None, None), P("dp", "tp", None, None), P("dp", None, "tp"), P("dp", "tp", None))
    return jax.shard_map(local_backward, mesh=mesh, in_specs=in_specs, out_specs=out_specs, check_vma=False)
```

```python
import functools

import jax
import jax.numpy as jnp
from jax import lax
from jax.experimental import pallas as pl
from jax.experimental.pallas import tpu as pltpu
from jax.sharding import PartitionSpec as P

RMS_EPS = 1e-6
f32 = jnp.float32
bf16 = jnp.bfloat16

OWN, T, W, O, PC, TP, WP, OP = range(8)
XOR = (0, 6, 2, 4, 1, 7, 3, 5)
CORE, NEAR_T, NEAR_W = 1, 6, 2
AG_SEMS = 11
RS_SEMS = 12
NN, NT, TN = ((1,), (0,)), ((1,), (1,)), ((0,), (0,))


def peer(mask):
    out = lax.axis_index("tp")
    for bit in (1, 2, 4):
        if mask & bit:
            out = out + bit - 2 * bit * (lax.rem(out, 2 * bit) // bit)
    return {"tp": out}


def greet(masks):
    for mask in masks:
        pl.semaphore_signal(pltpu.get_barrier_semaphore(), inc=1, device_id=peer(mask), device_id_type=pl.DeviceIdType.MESH)


def meet(masks):
    pl.semaphore_wait(pltpu.get_barrier_semaphore(), len(masks))


def remote(src, dst, send, recv, index, mask):
    return pltpu.make_async_remote_copy(
        src_ref=src, dst_ref=dst, send_sem=send.at[index], recv_sem=recv.at[index],
        device_id=peer(mask), device_id_type=pl.DeviceIdType.MESH)


def dot(left, right, dims):
    return lax.dot_general(left, right, (dims, ((), ())), preferred_element_type=f32)


def loop(count, body):
    def step(i, carry):
        body(i)
        return carry
    lax.fori_loop(0, count, step, 0)


def tiles(total, size, body):
    loop(total // size, lambda i: body(pl.ds(pl.multiple_of(i * size, size), size)))


class Gather:
    def __init__(self, buf, send, recv):
        rows = buf.shape[0] // 8
        half = rows // 2

        def at(block, lo=0, size=rows):
            return buf.at[pl.ds(block * rows + lo, size)]

        self.t_hi = remote(at(OWN, half, half), at(T, half, half), send, recv, 0, NEAR_T)
        self.t_lo = remote(at(OWN, 0, half), at(T, 0, half), send, recv, 9, NEAR_T)
        self.w_lo = remote(at(OWN, 0, half), at(W, 0, half), send, recv, 1, NEAR_W)
        self.w_hi = remote(at(OWN, half, half), at(W, half, half), send, recv, 10, NEAR_W)
        self.p = remote(at(OWN), at(PC), send, recv, 2, CORE)
        self.oa = remote(at(W, 0, half), at(O, 0, half), send, recv, 3, NEAR_T)
        self.ob = remote(at(T, half, half), at(O, half, half), send, recv, 4, NEAR_W)
        self.tp = remote(at(T), at(TP), send, recv, 5, CORE)
        self.wp = remote(at(W), at(WP), send, recv, 6, CORE)
        self.opa = remote(at(O, 0, half), at(OP, 0, half), send, recv, 7, CORE)
        self.opb = remote(at(O, half, half), at(OP, half, half), send, recv, 8, CORE)

    def start(self):
        for copy in (self.t_hi, self.w_lo, self.t_lo, self.w_hi, self.p):
            copy.start()

    def forward(self):
        self.t_hi.wait_recv()
        self.ob.start()
        self.w_lo.wait_recv()
        self.oa.start()

    def share(self):
        self.t_lo.wait_recv()
        self.tp.start()
        self.w_hi.wait_recv()
        self.wp.start()

    def finish(self):
        self.oa.wait_recv()
        self.opa.start()
        self.ob.wait_recv()
        self.opb.start()

    def last(self):
        self.opa.wait_recv()
        self.opb.wait_recv()

    def drain(self):
        for copy in (self.t_hi, self.t_lo, self.w_lo, self.w_hi, self.p, self.oa, self.ob, self.tp, self.wp, self.opa, self.opb):
            copy.wait_send()

    def each_block(self, compute, neighbours=None):
        def body(step):
            if neighbours is not None:
                pl.when(step == 2)(neighbours)
            for when, act in ((1, self.p.wait_recv), (3, self.tp.wait_recv), (5, self.wp.wait_recv), (6, self.finish), (7, self.last)):
                pl.when(step == when)(act)
            compute(step // 2 + 4 * lax.rem(step, 2))
        loop(8, body)


class Scatter:
    def __init__(self, part, bufs, send, recv):
        self.part, self.send, self.recv = part, send, recv
        self.snd, self.kept, self.in_o, self.in_w, self.in_t = bufs
        half = self.in_o.shape[0] // 2
        lo, hi = pl.ds(0, half), pl.ds(half, half)
        self.lo, self.hi = lo, hi
        self.oa = remote(self.kept.at[O, lo], self.in_o.at[lo], send, recv, 4, NEAR_T)
        self.ob = remote(self.kept.at[O, hi], self.in_o.at[hi], send, recv, 5, NEAR_W)
        self.w_hi = remote(self.kept.at[W, hi], self.in_w.at[hi], send, recv, 6, NEAR_W)
        self.t_lo = remote(self.kept.at[T, lo], self.in_t.at[lo], send, recv, 7, NEAR_T)
        quarter = half // 2
        self.quarter, self.half = quarter, half
        self.w_rows = [pl.ds(i * quarter, quarter) for i in range(2)]
        self.t_rows = [pl.ds(half + i * quarter, quarter) for i in range(2)]
        self.w_lo = [remote(self.kept.at[W, r], self.in_w.at[r], send, recv, 8 + i, NEAR_W) for i, r in enumerate(self.w_rows)]
        self.t_hi = [remote(self.kept.at[T, r], self.in_t.at[r], send, recv, 10 + i, NEAR_T) for i, r in enumerate(self.t_rows)]

    def d2d(self, i):
        return remote(self.snd.at[lax.rem(i, 2)], self.kept.at[3 - i], self.send, self.recv, i, CORE)

    def begin(self):
        self.theirs()
        self.mine()

    def theirs(self):
        def body(i):
            @pl.when(i >= 2)
            def _():
                self.d2d(i - 2).wait_send()
            self.part(7 - i, self.snd.at[lax.rem(i, 2)], False)
            self.d2d(i).start()
        loop(4, body)

    def mine(self):
        def body(i):
            self.d2d(i).wait_recv()
            self.part(3 - i, self.kept.at[3 - i], True)

            @pl.when(i == 0)
            def _():
                self.oa.start()
                self.ob.start()
            pl.when(i == 1)(self.w_hi.start)
            pl.when(i == 2)(self.t_lo.start)
        loop(4, body)

    def middle(self):
        self.oa.wait_recv()
        for rows, copy in zip(self.w_rows, self.w_lo):
            self.kept[W, rows] = self.kept[W, rows] + self.in_o[rows]
            copy.start()
        self.ob.wait_recv()
        for rows, copy in zip(self.t_rows, self.t_hi):
            self.kept[T, rows] = self.kept[T, rows] + self.in_o[rows]
            copy.start()

    def each_tile(self, apply):
        self.w_hi.wait_recv()
        self.t_lo.wait_recv()
        for i in range(2):
            self.w_lo[i].wait_recv()
            self.t_hi[i].wait_recv()
            for base in (i * self.quarter, self.half + i * self.quarter):
                def body(k):
                    start = pl.multiple_of(base + k * ROW_TILE, ROW_TILE)
                    here = pl.ds(start, ROW_TILE)
                    apply(start, self.kept[OWN, here] + self.in_w[here] + self.in_t[here])
                loop(self.quarter // ROW_TILE, body)

    def drain(self, slots=True):
        if slots:
            self.free_slots()
        for copy in (self.oa, self.ob, self.w_hi, self.t_lo, *self.w_lo, *self.t_hi):
            copy.wait_send()

    def free_slots(self):
        self.d2d(2).wait_send()
        self.d2d(3).wait_send()


ROW_TILE = 32


def inv_rms_of(tensor):
    return lax.rsqrt(jnp.mean(tensor * tensor, axis=-1, keepdims=True) + RMS_EPS)


def rms_norm(tensor):
    return tensor * inv_rms_of(tensor)


def rms_back(tensor, grad_in):
    inv_rms = inv_rms_of(tensor)
    return inv_rms * grad_in - tensor * (inv_rms * inv_rms * inv_rms) * jnp.mean(grad_in * tensor, axis=-1, keepdims=True)


def gelu_tanh(tensor):
    return jax.nn.gelu(tensor, approximate=True)


def mlp_kernel(layer, n_held, *refs):
    mlp_body(layer, *refs[:6], *refs[6 + n_held:])


def mlp_body(layer, y1_hbm, dy2_hbm, y2_hbm, dy1_hbm, w1_hbm, w2_hbm, x2_out, dy1_out, dw1_hbm, dw2_hbm,
             y1, w1, w2, u_all, c_all, act, hid, dpre, tmp, dw1, dw2,
               g_snd, g_kept, g_o, g_w, g_t, d_snd, d_kept, d_o, d_w, d_t,
               us, ur, cs, cr, gs, gr, ds, dr, local):
    rows, hidden = y1.shape
    cols = w1.shape[1]
    near = (CORE, NEAR_T, NEAR_W)
    greet(near)
    get_y1 = pltpu.make_async_copy(y1_hbm, y1, local.at[2])
    get_dy2 = pltpu.make_async_copy(dy2_hbm, dy1_out, local.at[3])
    get_y2 = pltpu.make_async_copy(y2_hbm, x2_out, local.at[4])
    get_dy1 = pltpu.make_async_copy(dy1_hbm, dy1_out, local.at[5])
    get_w1 = pltpu.make_async_copy(w1_hbm.at[layer], w1, local.at[0])
    get_w2 = pltpu.make_async_copy(w2_hbm.at[layer], w2, local.at[1])
    for copy in (get_y1, get_dy2, get_w1, get_w2, get_y2):
        copy.start()
    gu = Gather(u_all, us, ur)
    gc = Gather(c_all, cs, cr)

    def block_rows(block):
        return pl.ds(pl.multiple_of(block * rows, rows), rows)

    get_y1.wait()

    def norm_in(here):
        u_all[here] = rms_norm(y1[here]).astype(bf16)
    tiles(rows, ROW_TILE, norm_in)
    meet(near)
    gu.start()

    get_dy2.wait()

    def cast_in(here):
        c_all[here] = dy1_out[here].astype(bf16)
    tiles(rows, ROW_TILE, cast_in)
    get_dy1.start()
    get_w1.wait()
    get_w2.wait()

    def up(block):
        here = block_rows(block)
        act[here] = dot(u_all[here], w1[...], NN)

        def body(i):
            some = pl.ds(pl.multiple_of(block * rows + i * ROW_TILE, ROW_TILE), ROW_TILE)
            hid[some] = gelu_tanh(act[some]).astype(bf16)
        loop(rows // ROW_TILE, body)

    def down(block):
        tmp[...] = dot(c_all[block_rows(block)], w2[...], NT)

        def body(i):
            some = pl.ds(pl.multiple_of(block * rows + i * ROW_TILE, ROW_TILE), ROW_TILE)
            _, pull = jax.vjp(gelu_tanh, act[some])
            dpre[some] = pull(tmp[pl.ds(pl.multiple_of(i * ROW_TILE, ROW_TILE), ROW_TILE)])[0].astype(bf16)
        loop(rows // ROW_TILE, body)

    def part_of(lhs, rhs, transposed):
        def part(block, out, accumulate):
            here = block_rows(block)

            def body(col):
                value = dot(lhs[here], rhs[col, :], NT) if transposed else dot(lhs[here], rhs[:, col], NN)
                out[:, col] = out[:, col] + value if accumulate else value
            tiles(hidden, 256, body)
        return part

    rs_g = Scatter(part_of(hid, w2, False), (g_snd, g_kept, g_o, g_w, g_t), gs, gr)
    rs_d = Scatter(part_of(dpre, w1, True), (d_snd, d_kept, d_o, d_w, d_t), ds, dr)

    def u_neighbours():
        gu.forward()
        gu.share()
        gc.start()

    def c_neighbours():
        gc.share()
        rs_g.mine()
    gu.each_block(up, u_neighbours)
    rs_g.theirs()
    gc.forward()
    gc.each_block(down, c_neighbours)
    rs_g.middle()
    rs_d.begin()

    def body2(col):
        dw2[col, :] = dot(hid[:, col], c_all[...], TN)
    tiles(cols, 128, body2)
    put_dw2 = pltpu.make_async_copy(dw2, dw2_hbm.at[layer], local.at[0])
    put_dw2.start()
    rs_d.middle()
    get_y2.wait()

    def x2_body(start, total):
        here = pl.ds(start, ROW_TILE)
        x2_out[here] = x2_out[here] - total
    rs_g.each_tile(x2_body)

    def body1(col):
        dw1[col, :] = dot(u_all[:, col], dpre[...], TN)
    tiles(hidden, 256, body1)
    put_dw1 = pltpu.make_async_copy(dw1, dw1_hbm.at[layer], local.at[1])
    put_dw1.start()
    get_dy1.wait()

    def dy1_body(start, total):
        here = pl.ds(start, ROW_TILE)
        dy1_out[here] = dy1_out[here] + rms_back(y1[here], total)
    rs_d.each_tile(dy1_body)
    gu.drain()
    gc.drain()
    rs_g.drain()
    rs_d.drain()
    put_dw2.wait()
    put_dw1.wait()


def attn_kernel(layer, scale, n_held, *refs):
    attn_body(layer, scale, *refs[:6], *refs[6 + n_held:])


def attn_body(layer, scale, x2_hbm, dy1_hbm, y1_hbm, dy2_hbm, wqkv_hbm, wo_hbm, x1_out, dx2_out, dwqkv_hbm, dwo_hbm, x2, dwqkv, dwo,
                wq, wk, wv, wo_all, u_all, c_all, q_all, k_all, v_all, dctx, ctx, packed, ctx_in, others_ctx, relay, prob,
                a_snd, a_kept, a_o, a_w, a_t, b_snd, b_kept, b_o, b_w, b_t,
                us, ur, cs, cr, ws, wr, xs, xr, as_, ar, bs, br, local):
    rows, hidden = x2.shape
    width = wq.shape[0]
    head = width // 2
    pos = 32
    n_seq = rows // pos
    greet(XOR[1:])
    get_x2 = pltpu.make_async_copy(x2_hbm, x2, local.at[7])
    get_dy1 = pltpu.make_async_copy(dy1_hbm, dx2_out, local.at[8])
    get_dy2 = pltpu.make_async_copy(dy2_hbm, dx2_out, local.at[9])
    get_y1 = pltpu.make_async_copy(y1_hbm, x1_out, local.at[10])
    get_x2.start()
    get_dy1.start()
    gets = []
    for n in range(2):
        for j, ref in enumerate((wq, wk, wv)):
            gets.append(pltpu.make_async_copy(wqkv_hbm.at[layer, n, j], ref.at[pl.ds(n * head, head)], local.at[len(gets)]))
    gets.append(pltpu.make_async_copy(wo_hbm.at[layer], wo_all.at[pl.ds(0, width)], local.at[len(gets)]))
    for copy in gets:
        copy.start()
    gu = Gather(u_all, us, ur)
    gc = Gather(c_all, cs, cr)
    gw = Gather(wo_all, ws, wr)
    lanes = lax.broadcasted_iota(jnp.int32, (1, width), 1)
    masks = [(lanes < head), (lanes >= head)]

    get_x2.wait()

    def norm_in(here):
        u_all[here] = rms_norm(x2[here]).astype(bf16)
    tiles(rows, ROW_TILE, norm_in)
    meet(XOR[1:])
    gu.start()

    get_dy1.wait()

    def cast_in(here):
        c_all[here] = dx2_out[here].astype(bf16)
    tiles(rows, ROW_TILE, cast_in)
    get_dy2.start()
    get_y1.start()
    for copy in gets:
        copy.wait()

    def block_rows(block):
        return pl.ds(pl.multiple_of(block * rows, rows), rows)

    def pick(value, n):
        return jnp.where(masks[n], value, jnp.zeros_like(value))

    def qkv(block):
        here = block_rows(block)
        value = u_all[here]
        for weight, out in ((wq, q_all), (wk, k_all), (wv, v_all)):
            out[here] = dot(value, weight[...], NT).astype(bf16)

    def d_ctx(block):
        here = block_rows(block)
        dctx[here] = dot(c_all[here], wo_all[pl.ds(0, width)], NT).astype(bf16)

    def seq_get(ref, seq):
        return jnp.concatenate([ref[pl.ds(pl.multiple_of(b * rows + seq * pos, pos), pos)] for b in range(8)], axis=0)

    def seq_put(ref, seq, value):
        for b in range(8):
            ref[pl.ds(pl.multiple_of(b * rows + seq * pos, pos), pos)] = value[b * pos:(b + 1) * pos]

    def forward(seq):
        q, k, v = seq_get(q_all, seq), seq_get(k_all, seq), seq_get(v_all, seq)
        total = None
        for n in range(2):
            scores = dot(pick(q, n), k, NT) * scale
            expd = jnp.exp(scores - jnp.max(scores, axis=-1, keepdims=True))
            p = expd / jnp.sum(expd, axis=-1, keepdims=True)
            prob[2 * seq + n] = p
            out = dot(p.astype(bf16), pick(v, n), NN)
            total = out if total is None else total + out
        seq_put(ctx, seq, total.astype(bf16))

    def backward(seq):
        q, k, v, do = seq_get(q_all, seq), seq_get(k_all, seq), seq_get(v_all, seq), seq_get(dctx, seq)
        sums = [None, None, None]
        for n in range(2):
            p = prob[2 * seq + n]
            dp = dot(pick(do, n), v, NT)
            d_value = dot(p.astype(bf16), pick(do, n), TN)
            dsc = (p * (dp - jnp.sum(dp * p, axis=-1, keepdims=True)) * scale).astype(bf16)
            terms = [dot(dsc, pick(k, n), NN), dot(dsc, pick(q, n), TN), d_value]
            sums = [b if a is None else a + b for a, b in zip(sums, terms)]
        for ref, value in zip((q_all, k_all, v_all), sums):
            seq_put(ref, seq, value.astype(bf16))

    half = rows // 2

    def part_of(chunk):
        def part(block, out, accumulate):
            here = pl.ds(pl.multiple_of(block * rows + chunk * half, half), half)

            def body(col):
                value = dot(q_all[here], wq[:, col], NN) + dot(k_all[here], wk[:, col], NN) + dot(v_all[here], wv[:, col], NN)
                out[:, col] = out[:, col] + value if accumulate else value
            tiles(hidden, 256, body)
        return part

    rs_a = Scatter(part_of(0), (a_snd, a_kept, a_o, a_w, a_t), as_, ar)
    rs_b = Scatter(part_of(1), (b_snd, b_kept, b_o, b_w, b_t), bs, br)
    shares = [remote(packed.at[b], ctx_in.at[b], xs, xr, i, XOR[b])
              for i, b in enumerate((T, W, PC, TP, WP))]
    via, onward = [], []
    split = packed.shape[1] // 2
    for i, (row, near, others) in enumerate(((0, NEAR_T, (2, 3)), (split, NEAR_W, (6, 7)))):
        for j, b in enumerate((O, OP)):
            slot = 2 * i + j
            via.append(remote(packed.at[b, pl.ds(row, split)], relay.at[slot], xs, xr, 5 + slot, near))
            onward.append(remote(relay.at[slot], ctx_in.at[b, pl.ds(row, split)], xs, xr, 9 + slot, others[j]))

    def u_neighbours():
        gu.forward()
        gu.share()
        gc.start()
    gu.each_block(qkv, u_neighbours)
    loop(n_seq // 2, forward)
    gc.forward()
    loop(n_seq // 2, lambda i: forward(i + n_seq // 2))
    extra = width - 128
    group = rows * extra // 128

    def pack(b):
        value = ctx[block_rows(b)]
        packed[b, pl.ds(0, rows)] = value[:, :128]
        packed[b, pl.ds(rows, group)] = jnp.concatenate(
            [value[i * group:(i + 1) * group, 128:] for i in range(rows // group)], axis=1)

    def unpack(i):
        b = i + 1
        rest = ctx_in[b, pl.ds(rows, group)]
        rest = jnp.concatenate([rest[:, j * extra:(j + 1) * extra] for j in range(rows // group)], axis=0)
        others_ctx[b] = jnp.concatenate([ctx_in[b, pl.ds(0, rows)], rest], axis=1)
    loop(8, pack)
    gc.share()
    for copy in via + shares:
        copy.start()
    gw.start()
    gc.each_block(d_ctx)
    for first, second in zip(via, onward):
        first.wait_recv()
        second.start()
    loop(n_seq // 2, backward)
    gw.forward()
    rs_a.begin()
    gw.share()
    loop(n_seq // 2, lambda i: backward(i + n_seq // 2))
    rs_a.middle()
    rs_b.begin()
    dwo[...] = dot(ctx[...], c_all[...], TN)
    gw.finish()
    for i, ref in enumerate((q_all, k_all, v_all)):
        grad = dot(ref[...], u_all[...], TN)
        for n in range(2):
            dwqkv[n, i] = grad[n * head:(n + 1) * head]
    puts = [pltpu.make_async_copy(dwqkv, dwqkv_hbm.at[layer], local.at[0]),
            pltpu.make_async_copy(dwo, dwo_hbm.at[layer], local.at[1])]
    for copy in puts:
        copy.start()
    rs_b.middle()
    for copy in shares + onward:
        copy.wait_recv()
    for copy in (gw.p, gw.tp, gw.wp):
        copy.wait_recv()
    gw.last()

    loop(7, unpack)
    get_y1.wait()

    def f_body(col):
        total = dot(ctx[pl.ds(0, rows)], wo_all[pl.ds(0, width), col], NN)
        for b in range(1, 8):
            total = total + dot(others_ctx[b], wo_all[pl.ds(b * width, width), col], NN)
        x1_out[:, col] = x1_out[:, col] - total
    tiles(hidden, 256, f_body)
    get_dy2.wait()
    for chunk, item in enumerate((rs_a, rs_b)):
        def dx_body(start, total):
            here = pl.ds(pl.multiple_of(chunk * half + start, ROW_TILE), ROW_TILE)
            dx2_out[here] = dx2_out[here] + rms_back(x2[here], total)
        item.each_tile(dx_body)
    for item in (gu, gc, gw, rs_a, rs_b):
        item.drain()
    for copy in shares + via + onward:
        copy.wait_send()
    for copy in puts:
        copy.wait()


def vmem(shape, dtype):
    return pltpu.VMEM(shape, dtype)


def scatter_scratch(rows, hidden):
    return [vmem((2, rows, hidden), f32), vmem((4, rows, hidden), f32)] + [vmem((rows, hidden), f32)] * 3


def sems(count):
    return [pltpu.SemaphoreType.DMA((count,))] * 2


def call(kernel, outs, scratch, collective_id, name, flops, args, held):
    inside, outside = pl.BlockSpec(memory_space=pltpu.VMEM), pl.BlockSpec(memory_space=pl.ANY)
    return pl.pallas_call(
        kernel,
        out_shape=[jax.ShapeDtypeStruct(shape, f32) for shape, _ in outs],
        in_specs=[outside] * len(args + held),
        input_output_aliases={len(args) + i: 2 + i for i in range(len(held))},
        out_specs=[inside if kept else outside for _, kept in outs],
        scratch_shapes=scratch,
        name=name,
        cost_estimate=pl.CostEstimate(flops=flops, bytes_accessed=10 ** 7, transcendentals=0),
        compiler_params=pltpu.CompilerParams(
            collective_id=collective_id, has_side_effects=True, vmem_limit_bytes=67043328),
    )(*args, *held)


def mlp_block(layer, y1, dy2, y2, dy1, w1, w2, held):
    rows, hidden = y1.shape
    cols = w1.shape[2]
    total = 8 * rows
    scratch = [vmem((rows, hidden), f32), vmem((hidden, cols), bf16), vmem((cols, hidden), bf16)]
    scratch += [vmem((total, hidden), bf16)] * 2 + [vmem((total, cols), f32)] + [vmem((total, cols), bf16)] * 2
    scratch += [vmem((rows, cols), f32), vmem((hidden, cols), f32), vmem((cols, hidden), f32)]
    scratch += scatter_scratch(rows, hidden) * 2 + sems(AG_SEMS) * 2 + sems(RS_SEMS) * 2 + sems(6)[:1]
    outs = [((rows, hidden), True)] * 2 + [(w1.shape, False), (w2.shape, False)]
    kernel = functools.partial(mlp_kernel, layer, len(held))
    return call(kernel, outs, scratch, 2 * layer, "mlp_block", 12 * total * hidden * cols, (y1, dy2, y2, dy1, w1, w2), held)


def attn_block(layer, scale, x2, dy1, y1, dy2, wqkv, wo, held):
    rows, hidden = x2.shape
    _, heads, _, head, _ = wqkv.shape
    width = heads * head
    total = 8 * rows
    scratch = [vmem((rows, hidden), f32), vmem((heads, 3, head, hidden), f32), vmem((width, hidden), f32)] + [vmem((width, hidden), bf16)] * 3 + [vmem((8 * width, hidden), bf16)] + [vmem((total, hidden), bf16)] * 2
    scratch += [vmem((total, width), bf16)] * 5 + [vmem((8, rows * width // 128, 128), bf16)] * 2
    scratch += [vmem((8, rows, width), bf16), vmem((4, rows * width // 256, 128), bf16), vmem((16, 256, 256), f32)]
    scratch += scatter_scratch(rows // 2, hidden) * 2 + sems(AG_SEMS) * 3 + sems(13) + sems(RS_SEMS) * 2 + sems(11)[:1]
    outs = [((rows, hidden), True)] * 2 + [(wqkv.shape, False), (wo.shape, False)]
    kernel = functools.partial(attn_kernel, layer, scale, len(held))
    return call(kernel, outs, scratch, 2 * layer + 1, "attn_block", 24 * total * hidden * width, (x2, dy1, y1, dy2, wqkv, wo), held)


def local_backward(y_one, y_two, dy_one, dy_two, w_qkv, w_out, w_up, w_down):
    n_layers, hidden, heads, _, head_dim = w_qkv.shape
    state_shape = y_one.shape
    y_one, y_two, dy_one, dy_two = [x.reshape(-1, hidden) for x in (y_one, y_two, dy_one, dy_two)]
    w_qkv = w_qkv.transpose(0, 2, 3, 4, 1)
    w_out = w_out.reshape(n_layers, heads * head_dim, hidden)
    held_mlp, held_attn = (), ()
    for layer in reversed(range(n_layers)):
        y_two, dy_one, *held_mlp = mlp_block(layer, y_one, dy_two, y_two, dy_one, w_up, w_down, tuple(held_mlp))
        y_one, dy_two, *held_attn = attn_block(
            layer, head_dim ** -0.5, y_two, dy_one, y_one, dy_two, w_qkv, w_out, tuple(held_attn))
    d_qkv, d_out, d_up, d_down = *held_attn, *held_mlp
    state = [x.reshape(state_shape) for x in (y_one, y_two, dy_one, dy_two)]
    return (*state, d_qkv.transpose(0, 4, 1, 2, 3), d_out.reshape(n_layers, heads, head_dim, hidden), d_up, d_down)


def solution(mesh):
    state_spec = P("dp", "tp", None)
    in_specs = (state_spec, state_spec, state_spec, state_spec, P(None, None, "tp", None, None), P(None, "tp", None, None), P(None, None, "tp"), P(None, "tp", None))
    out_specs = (state_spec, state_spec, state_spec, state_spec, P("dp", None, "tp", None, None), P("dp", "tp", None, None), P("dp", None, "tp"), P("dp", "tp", None))
    return jax.shard_map(local_backward, mesh=mesh, in_specs=in_specs, out_specs=out_specs, check_vma=False)
```

```python
import functools

import jax
import jax.numpy as jnp
from jax import lax
from jax.experimental import pallas as pl
from jax.experimental.pallas import tpu as pltpu
from jax.sharding import PartitionSpec as P

RMS_EPS = 1e-6
f32 = jnp.float32
bf16 = jnp.bfloat16

OWN, T, W, O, PC, TP, WP, OP = range(8)
XOR = (0, 6, 2, 4, 1, 7, 3, 5)
CORE, NEAR_T, NEAR_W = 1, 6, 2
AG_SEMS = 11
RS_SEMS = 12
NN, NT, TN = ((1,), (0,)), ((1,), (1,)), ((0,), (0,))


def peer(mask):
    out = lax.axis_index("tp")
    for bit in (1, 2, 4):
        if mask & bit:
            out = out + bit - 2 * bit * (lax.rem(out, 2 * bit) // bit)
    return {"tp": out}


def greet(masks):
    for mask in masks:
        pl.semaphore_signal(pltpu.get_barrier_semaphore(), inc=1, device_id=peer(mask), device_id_type=pl.DeviceIdType.MESH)


def meet(masks):
    pl.semaphore_wait(pltpu.get_barrier_semaphore(), len(masks))


def remote(src, dst, send, recv, index, mask):
    return pltpu.make_async_remote_copy(
        src_ref=src, dst_ref=dst, send_sem=send.at[index], recv_sem=recv.at[index],
        device_id=peer(mask), device_id_type=pl.DeviceIdType.MESH)


def dot(left, right, dims):
    return lax.dot_general(left, right, (dims, ((), ())), preferred_element_type=f32)


def loop(count, body):
    def step(i, carry):
        body(i)
        return carry
    lax.fori_loop(0, count, step, 0)


def tiles(total, size, body):
    loop(total // size, lambda i: body(pl.ds(pl.multiple_of(i * size, size), size)))


class Gather:
    def __init__(self, buf, send, recv):
        rows = buf.shape[0] // 8
        half = rows // 2

        def at(block, lo=0, size=rows):
            return buf.at[pl.ds(block * rows + lo, size)]

        self.t_hi = remote(at(OWN, half, half), at(T, half, half), send, recv, 0, NEAR_T)
        self.t_lo = remote(at(OWN, 0, half), at(T, 0, half), send, recv, 9, NEAR_T)
        self.w_lo = remote(at(OWN, 0, half), at(W, 0, half), send, recv, 1, NEAR_W)
        self.w_hi = remote(at(OWN, half, half), at(W, half, half), send, recv, 10, NEAR_W)
        self.p = remote(at(OWN), at(PC), send, recv, 2, CORE)
        self.oa = remote(at(W, 0, half), at(O, 0, half), send, recv, 3, NEAR_T)
        self.ob = remote(at(T, half, half), at(O, half, half), send, recv, 4, NEAR_W)
        self.tp = remote(at(T), at(TP), send, recv, 5, CORE)
        self.wp = remote(at(W), at(WP), send, recv, 6, CORE)
        self.opa = remote(at(O, 0, half), at(OP, 0, half), send, recv, 7, CORE)
        self.opb = remote(at(O, half, half), at(OP, half, half), send, recv, 8, CORE)

    def start(self):
        for copy in (self.t_hi, self.w_lo, self.t_lo, self.w_hi, self.p):
            copy.start()

    def forward(self):
        self.t_hi.wait_recv()
        self.ob.start()
        self.w_lo.wait_recv()
        self.oa.start()

    def share(self):
        self.t_lo.wait_recv()
        self.tp.start()
        self.w_hi.wait_recv()
        self.wp.start()

    def finish(self):
        self.oa.wait_recv()
        self.opa.start()
        self.ob.wait_recv()
        self.opb.start()

    def last(self):
        self.opa.wait_recv()
        self.opb.wait_recv()

    def drain(self):
        for copy in (self.t_hi, self.t_lo, self.w_lo, self.w_hi, self.p, self.oa, self.ob, self.tp, self.wp, self.opa, self.opb):
            copy.wait_send()

    def each_block(self, compute, neighbours=None):
        def body(step):
            if neighbours is not None:
                pl.when(step == 2)(neighbours)
            for when, act in ((1, self.p.wait_recv), (3, self.tp.wait_recv), (5, self.wp.wait_recv), (6, self.finish), (7, self.last)):
                pl.when(step == when)(act)
            compute(step // 2 + 4 * lax.rem(step, 2))
        loop(8, body)


class Scatter:
    def __init__(self, part, bufs, send, recv):
        self.part, self.send, self.recv = part, send, recv
        self.snd, self.kept, self.in_o, self.in_w, self.in_t = bufs
        half = self.in_o.shape[0] // 2
        lo, hi = pl.ds(0, half), pl.ds(half, half)
        self.lo, self.hi = lo, hi
        self.oa = remote(self.kept.at[O, lo], self.in_o.at[lo], send, recv, 4, NEAR_T)
        self.ob = remote(self.kept.at[O, hi], self.in_o.at[hi], send, recv, 5, NEAR_W)
        self.w_hi = remote(self.kept.at[W, hi], self.in_w.at[hi], send, recv, 6, NEAR_W)
        self.t_lo = remote(self.kept.at[T, lo], self.in_t.at[lo], send, recv, 7, NEAR_T)
        quarter = half // 2
        self.quarter, self.half = quarter, half
        self.w_rows = [pl.ds(i * quarter, quarter) for i in range(2)]
        self.t_rows = [pl.ds(half + i * quarter, quarter) for i in range(2)]
        self.w_lo = [remote(self.kept.at[W, r], self.in_w.at[r], send, recv, 8 + i, NEAR_W) for i, r in enumerate(self.w_rows)]
        self.t_hi = [remote(self.kept.at[T, r], self.in_t.at[r], send, recv, 10 + i, NEAR_T) for i, r in enumerate(self.t_rows)]

    def d2d(self, i):
        return remote(self.snd.at[lax.rem(i, 2)], self.kept.at[3 - i], self.send, self.recv, i, CORE)

    def begin(self):
        self.theirs()
        self.mine()

    def theirs(self):
        def body(i):
            @pl.when(i >= 2)
            def _():
                self.d2d(i - 2).wait_send()
            self.part(7 - i, self.snd.at[lax.rem(i, 2)], False)
            self.d2d(i).start()
        loop(4, body)

    def mine(self):
        def body(i):
            self.d2d(i).wait_recv()
            self.part(3 - i, self.kept.at[3 - i], True)

            @pl.when(i == 0)
            def _():
                self.oa.start()
                self.ob.start()
            pl.when(i == 1)(self.w_hi.start)
            pl.when(i == 2)(self.t_lo.start)
        loop(4, body)

    def middle(self):
        self.oa.wait_recv()
        for rows, copy in zip(self.w_rows, self.w_lo):
            self.kept[W, rows] = self.kept[W, rows] + self.in_o[rows]
            copy.start()
        self.ob.wait_recv()
        for rows, copy in zip(self.t_rows, self.t_hi):
            self.kept[T, rows] = self.kept[T, rows] + self.in_o[rows]
            copy.start()

    def each_tile(self, apply, done=lambda index, start, size: None):
        self.w_hi.wait_recv()
        self.t_lo.wait_recv()
        for i in range(2):
            self.w_lo[i].wait_recv()
            self.t_hi[i].wait_recv()
            for base in (i * self.quarter, self.half + i * self.quarter):
                def body(k):
                    start = pl.multiple_of(base + k * ROW_TILE, ROW_TILE)
                    here = pl.ds(start, ROW_TILE)
                    apply(start, self.kept[OWN, here] + self.in_w[here] + self.in_t[here])
                loop(self.quarter // ROW_TILE, body)
                done(2 * i + base // self.half, base, self.quarter)

    def drain(self, slots=True):
        if slots:
            self.free_slots()
        for copy in (self.oa, self.ob, self.w_hi, self.t_lo, *self.w_lo, *self.t_hi):
            copy.wait_send()

    def free_slots(self):
        self.d2d(2).wait_send()
        self.d2d(3).wait_send()


ROW_TILE = 32


def inv_rms_of(tensor):
    return lax.rsqrt(jnp.mean(tensor * tensor, axis=-1, keepdims=True) + RMS_EPS)


def rms_norm(tensor):
    return tensor * inv_rms_of(tensor)


def rms_back(tensor, grad_in):
    inv_rms = inv_rms_of(tensor)
    return inv_rms * grad_in - tensor * (inv_rms * inv_rms * inv_rms) * jnp.mean(grad_in * tensor, axis=-1, keepdims=True)


def gelu_tanh(tensor):
    return jax.nn.gelu(tensor, approximate=True)


def mlp_kernel(layer, first, n_held, *refs):
    count = 6 if first else 7
    u_hbm = None if first else refs[6]
    mlp_body(layer, u_hbm, *refs[:6], *refs[count + n_held:])


def mlp_body(layer, u_hbm, y1_hbm, dy2_hbm, y2_hbm, dy1_hbm, w1_hbm, w2_hbm, x2_hbm, dy1_new, dw1_hbm, dw2_hbm, u_new, x2_out, dy1_out, u_out,
             y1, w1, w2, u_all, c_all, act, hid, dpre, tmp, dw1, dw2,
               g_snd, g_kept, g_o, g_w, g_t, d_snd, d_kept, d_o, d_w, d_t,
               us, ur, cs, cr, gs, gr, ds, dr, local):
    rows, hidden = y1.shape
    cols = w1.shape[1]
    near = (CORE, NEAR_T, NEAR_W)
    greet(near)
    get_y1 = pltpu.make_async_copy(y1_hbm, y1, local.at[2])
    get_dy2 = pltpu.make_async_copy(dy2_hbm, dy1_out, local.at[3])
    get_y2 = pltpu.make_async_copy(y2_hbm, x2_out, local.at[4])
    get_dy1 = pltpu.make_async_copy(dy1_hbm, dy1_out, local.at[5])
    get_w1 = pltpu.make_async_copy(w1_hbm.at[layer], w1, local.at[0])
    get_w2 = pltpu.make_async_copy(w2_hbm.at[layer], w2, local.at[1])
    if u_hbm is not None:
        get_u = pltpu.make_async_copy(u_hbm, u_all.at[pl.ds(0, rows)], local.at[6])
        get_u.start()
    for copy in (get_y1, get_dy2, get_w1, get_w2, get_y2):
        copy.start()
    gu = Gather(u_all, us, ur)
    gc = Gather(c_all, cs, cr)

    def block_rows(block):
        return pl.ds(pl.multiple_of(block * rows, rows), rows)

    if u_hbm is None:
        get_y1.wait()

        def norm_in(here):
            u_all[here] = rms_norm(y1[here]).astype(bf16)
        tiles(rows, ROW_TILE, norm_in)
    else:
        get_u.wait()
    meet(near)
    gu.start()

    get_dy2.wait()

    def cast_in(here):
        c_all[here] = dy1_out[here].astype(bf16)
    tiles(rows, ROW_TILE, cast_in)
    get_dy1.start()
    get_w1.wait()
    get_w2.wait()

    def up(block):
        here = block_rows(block)
        act[here] = dot(u_all[here], w1[...], NN)

        def body(i):
            some = pl.ds(pl.multiple_of(block * rows + i * ROW_TILE, ROW_TILE), ROW_TILE)
            hid[some] = gelu_tanh(act[some]).astype(bf16)
        loop(rows // ROW_TILE, body)

    def down(block):
        tmp[...] = dot(c_all[block_rows(block)], w2[...], NT)

        def body(i):
            some = pl.ds(pl.multiple_of(block * rows + i * ROW_TILE, ROW_TILE), ROW_TILE)
            _, pull = jax.vjp(gelu_tanh, act[some])
            dpre[some] = pull(tmp[pl.ds(pl.multiple_of(i * ROW_TILE, ROW_TILE), ROW_TILE)])[0].astype(bf16)
        loop(rows // ROW_TILE, body)

    def part_of(lhs, rhs, transposed):
        def part(block, out, accumulate):
            here = block_rows(block)

            def body(col):
                value = dot(lhs[here], rhs[col, :], NT) if transposed else dot(lhs[here], rhs[:, col], NN)
                out[:, col] = out[:, col] + value if accumulate else value
            tiles(hidden, 256, body)
        return part

    rs_g = Scatter(part_of(hid, w2, False), (g_snd, g_kept, g_o, g_w, g_t), gs, gr)
    rs_d = Scatter(part_of(dpre, w1, True), (d_snd, d_kept, d_o, d_w, d_t), ds, dr)

    def u_neighbours():
        gu.forward()
        gu.share()
        gc.start()

    def c_neighbours():
        gc.share()
        rs_g.mine()
    gu.each_block(up, u_neighbours)
    rs_g.theirs()
    gc.forward()
    gc.each_block(down, c_neighbours)
    rs_g.middle()
    rs_d.begin()

    def body2(col):
        dw2[col, :] = dot(hid[:, col], c_all[...], TN)
    tiles(cols, 128, body2)
    put_dw2 = pltpu.make_async_copy(dw2, dw2_hbm.at[layer], local.at[0])
    put_dw2.start()
    rs_d.middle()
    get_y2.wait()
    if u_hbm is not None:
        get_y1.wait()

    def x2_body(start, total):
        here = pl.ds(start, ROW_TILE)
        x2 = x2_out[here] - total
        x2_out[here] = x2
        u_out[here] = rms_norm(x2).astype(bf16)
    rs_g.each_tile(x2_body)
    puts = [pltpu.make_async_copy(x2_out, x2_hbm, local.at[2]), pltpu.make_async_copy(u_out, u_new, local.at[3])]
    for copy in puts:
        copy.start()

    def body1(col):
        dw1[col, :] = dot(u_all[:, col], dpre[...], TN)
    tiles(hidden, 256, body1)
    put_dw1 = pltpu.make_async_copy(dw1, dw1_hbm.at[layer], local.at[1])
    put_dw1.start()
    get_dy1.wait()

    def dy1_body(start, total):
        here = pl.ds(start, ROW_TILE)
        dy1_out[here] = dy1_out[here] + rms_back(y1[here], total)

    def dy1_done(index, start, size):
        here = pl.ds(start, size)
        puts.append(pltpu.make_async_copy(dy1_out.at[here], dy1_new.at[here], local.at[7 + index]))
        puts[-1].start()
    rs_d.each_tile(dy1_body, dy1_done)
    gu.drain()
    gc.drain()
    rs_g.drain()
    rs_d.drain()
    for copy in (put_dw2, put_dw1, *puts):
        copy.wait()


def attn_kernel(layer, scale, last, n_held, *refs):
    rest = refs[7 + n_held:]
    outs = rest[:4] + ((None,) if last else rest[4:5])
    attn_body(layer, scale, *refs[:7], *outs, *rest[4 if last else 5:])


def attn_body(layer, scale, x2_hbm, dy1_hbm, y1_hbm, dy2_hbm, wqkv_hbm, wo_hbm, u_hbm, x1_hbm, dx2_hbm, dwqkv_hbm, dwo_hbm, u_new, x1_out, dx2_out, u_out, x2, dwqkv, dwo,
                wq, wk, wv, wo_all, u_all, c_all, q_all, k_all, v_all, dctx, ctx, packed, ctx_in, others_ctx, relay, prob,
                a_snd, a_kept, a_o, a_w, a_t, b_snd, b_kept, b_o, b_w, b_t,
                us, ur, cs, cr, ws, wr, xs, xr, as_, ar, bs, br, local):
    rows, hidden = x2.shape
    width = wq.shape[0]
    head = width // 2
    pos = 32
    n_seq = rows // pos
    met = [XOR[b] for b in (T, W, PC, TP, WP)]
    greet(met)
    get_x2 = pltpu.make_async_copy(x2_hbm, x2, local.at[7])
    get_dy1 = pltpu.make_async_copy(dy1_hbm, dx2_out, local.at[8])
    get_dy2 = pltpu.make_async_copy(dy2_hbm, dx2_out, local.at[9])
    get_y1 = pltpu.make_async_copy(y1_hbm, x1_out, local.at[10])
    get_u = pltpu.make_async_copy(u_hbm, u_all.at[pl.ds(0, rows)], local.at[11])
    for copy in (get_u, get_dy1, get_x2):
        copy.start()
    gets = []
    for n in range(2):
        for j, ref in enumerate((wq, wk, wv)):
            gets.append(pltpu.make_async_copy(wqkv_hbm.at[layer, n, j], ref.at[pl.ds(n * head, head)], local.at[len(gets)]))
    gets.append(pltpu.make_async_copy(wo_hbm.at[layer], wo_all.at[pl.ds(0, width)], local.at[len(gets)]))
    for copy in gets:
        copy.start()
    gu = Gather(u_all, us, ur)
    gc = Gather(c_all, cs, cr)
    gw = Gather(wo_all, ws, wr)
    lanes = lax.broadcasted_iota(jnp.int32, (1, width), 1)
    masks = [(lanes < head), (lanes >= head)]

    get_u.wait()
    meet(met)
    gu.start()

    get_dy1.wait()

    def cast_in(here):
        c_all[here] = dx2_out[here].astype(bf16)
    tiles(rows, ROW_TILE, cast_in)
    get_dy2.start()
    get_y1.start()
    for copy in gets:
        copy.wait()

    def block_rows(block):
        return pl.ds(pl.multiple_of(block * rows, rows), rows)

    def pick(value, n):
        return jnp.where(masks[n], value, jnp.zeros_like(value))

    def qkv(block):
        here = block_rows(block)
        value = u_all[here]
        for weight, out in ((wq, q_all), (wk, k_all), (wv, v_all)):
            out[here] = dot(value, weight[...], NT).astype(bf16)

    def d_ctx(block):
        here = block_rows(block)
        dctx[here] = dot(c_all[here], wo_all[pl.ds(0, width)], NT).astype(bf16)

    def seq_get(ref, seq):
        return jnp.concatenate([ref[pl.ds(pl.multiple_of(b * rows + seq * pos, pos), pos)] for b in range(8)], axis=0)

    def seq_put(ref, seq, value):
        for b in range(8):
            ref[pl.ds(pl.multiple_of(b * rows + seq * pos, pos), pos)] = value[b * pos:(b + 1) * pos]

    def forward(seq):
        q, k, v = seq_get(q_all, seq), seq_get(k_all, seq), seq_get(v_all, seq)
        total = None
        for n in range(2):
            scores = dot(pick(q, n), k, NT) * scale
            expd = jnp.exp(scores - jnp.max(scores, axis=-1, keepdims=True))
            p = expd / jnp.sum(expd, axis=-1, keepdims=True)
            prob[2 * seq + n] = p
            out = dot(p.astype(bf16), pick(v, n), NN)
            total = out if total is None else total + out
        seq_put(ctx, seq, total.astype(bf16))

    def backward(seq):
        q, k, v, do = seq_get(q_all, seq), seq_get(k_all, seq), seq_get(v_all, seq), seq_get(dctx, seq)
        sums = [None, None, None]
        for n in range(2):
            p = prob[2 * seq + n]
            dp = dot(pick(do, n), v, NT)
            d_value = dot(p.astype(bf16), pick(do, n), TN)
            dsc = (p * (dp - jnp.sum(dp * p, axis=-1, keepdims=True)) * scale).astype(bf16)
            terms = [dot(dsc, pick(k, n), NN), dot(dsc, pick(q, n), TN), d_value]
            sums = [b if a is None else a + b for a, b in zip(sums, terms)]
        for ref, value in zip((q_all, k_all, v_all), sums):
            seq_put(ref, seq, value.astype(bf16))

    half = rows // 2

    def part_of(chunk):
        def part(block, out, accumulate):
            here = pl.ds(pl.multiple_of(block * rows + chunk * half, half), half)

            def body(col):
                value = dot(q_all[here], wq[:, col], NN) + dot(k_all[here], wk[:, col], NN) + dot(v_all[here], wv[:, col], NN)
                out[:, col] = out[:, col] + value if accumulate else value
            tiles(hidden, 256, body)
        return part

    rs_a = Scatter(part_of(0), (a_snd, a_kept, a_o, a_w, a_t), as_, ar)
    rs_b = Scatter(part_of(1), (b_snd, b_kept, b_o, b_w, b_t), bs, br)
    shares = [remote(packed.at[b], ctx_in.at[b], xs, xr, i, XOR[b])
              for i, b in enumerate((T, W, PC, TP, WP))]
    via, onward = [], []
    split = packed.shape[1] // 2
    for i, (row, near, others) in enumerate(((0, NEAR_T, (2, 3)), (split, NEAR_W, (6, 7)))):
        for j, b in enumerate((O, OP)):
            slot = 2 * i + j
            via.append(remote(packed.at[b, pl.ds(row, split)], relay.at[slot], xs, xr, 5 + slot, near))
            onward.append(remote(relay.at[slot], ctx_in.at[b, pl.ds(row, split)], xs, xr, 9 + slot, others[j]))

    def u_neighbours():
        gu.forward()
        gu.share()
        gc.start()
    gu.each_block(qkv, u_neighbours)
    loop(n_seq // 2, forward)
    gc.forward()
    loop(n_seq // 2, lambda i: forward(i + n_seq // 2))
    extra = width - 128
    group = rows * extra // 128

    def pack(b):
        value = ctx[block_rows(b)]
        packed[b, pl.ds(0, rows)] = value[:, :128]
        packed[b, pl.ds(rows, group)] = jnp.concatenate(
            [value[i * group:(i + 1) * group, 128:] for i in range(rows // group)], axis=1)

    def unpack(i):
        b = i + 1
        rest = ctx_in[b, pl.ds(rows, group)]
        rest = jnp.concatenate([rest[:, j * extra:(j + 1) * extra] for j in range(rows // group)], axis=0)
        others_ctx[b] = jnp.concatenate([ctx_in[b, pl.ds(0, rows)], rest], axis=1)
    loop(8, pack)
    gc.share()
    for copy in via + shares:
        copy.start()
    gw.start()
    gc.each_block(d_ctx)
    for first, second in zip(via, onward):
        first.wait_recv()
        second.start()
    loop(n_seq // 2, backward)
    gw.forward()
    rs_a.begin()
    gw.share()
    loop(n_seq // 2, lambda i: backward(i + n_seq // 2))
    rs_a.middle()
    rs_b.begin()
    dwo[...] = dot(ctx[...], c_all[...], TN)
    gw.finish()
    for i, ref in enumerate((q_all, k_all, v_all)):
        grad = dot(ref[...], u_all[...], TN)
        for n in range(2):
            dwqkv[n, i] = grad[n * head:(n + 1) * head]
    puts = [pltpu.make_async_copy(dwqkv, dwqkv_hbm.at[layer], local.at[0]),
            pltpu.make_async_copy(dwo, dwo_hbm.at[layer], local.at[1])]
    for copy in puts:
        copy.start()
    rs_b.middle()
    for copy in shares + onward:
        copy.wait_recv()
    for copy in (gw.p, gw.tp, gw.wp):
        copy.wait_recv()
    gw.last()

    loop(7, unpack)
    get_y1.wait()

    def f_body(col):
        total = dot(ctx[pl.ds(0, rows)], wo_all[pl.ds(0, width), col], NN)
        for b in range(1, 8):
            total = total + dot(others_ctx[b], wo_all[pl.ds(b * width, width), col], NN)
        x1_out[:, col] = x1_out[:, col] - total
    tiles(hidden, 256, f_body)
    puts.append(pltpu.make_async_copy(x1_out, x1_hbm, local.at[2]))
    puts[-1].start()
    if u_new is not None:
        def norm_out(here):
            u_out[here] = rms_norm(x1_out[here]).astype(bf16)
        tiles(rows, ROW_TILE, norm_out)
        puts.append(pltpu.make_async_copy(u_out, u_new, local.at[3]))
        puts[-1].start()
    get_x2.wait()
    get_dy2.wait()
    for chunk, item in enumerate((rs_a, rs_b)):
        def dx_body(start, total):
            here = pl.ds(pl.multiple_of(chunk * half + start, ROW_TILE), ROW_TILE)
            dx2_out[here] = dx2_out[here] + rms_back(x2[here], total)

        def dx_done(index, start, size):
            here = pl.ds(chunk * half + start, size)
            puts.append(pltpu.make_async_copy(dx2_out.at[here], dx2_hbm.at[here], local.at[12 + 4 * chunk + index]))
            puts[-1].start()
        item.each_tile(dx_body, dx_done)
    for item in (gu, gc, gw, rs_a, rs_b):
        item.drain()
    for copy in shares + via + onward:
        copy.wait_send()
    for copy in puts:
        copy.wait()


def vmem(shape, dtype):
    return pltpu.VMEM(shape, dtype)


def scatter_scratch(rows, hidden):
    return [vmem((2, rows, hidden), f32), vmem((4, rows, hidden), f32)] + [vmem((rows, hidden), f32)] * 3


def sems(count):
    return [pltpu.SemaphoreType.DMA((count,))] * 2


def call(kernel, outs, scratch, collective_id, name, flops, limit, args, held):
    inside, outside = pl.BlockSpec(memory_space=pltpu.VMEM), pl.BlockSpec(memory_space=pl.ANY)
    return pl.pallas_call(
        kernel,
        out_shape=[jax.ShapeDtypeStruct(shape, dtype) for shape, _, dtype in outs],
        in_specs=[outside] * len(args + held),
        input_output_aliases={len(args) + i: 2 + i for i in range(len(held))},
        out_specs=[inside if kept else outside for _, kept, _ in outs],
        scratch_shapes=scratch,
        name=name,
        cost_estimate=pl.CostEstimate(flops=flops, bytes_accessed=10 ** 7, transcendentals=0),
        compiler_params=pltpu.CompilerParams(
            collective_id=collective_id, has_side_effects=True, vmem_limit_bytes=limit),
    )(*args, *held)


def mlp_block(layer, u, y1, dy2, y2, dy1, w1, w2, held):
    rows, hidden = y1.shape
    cols = w1.shape[2]
    total = 8 * rows
    scratch = [vmem((rows, hidden), f32)] * 2 + [vmem((rows, hidden), bf16)]
    scratch += [vmem((rows, hidden), f32), vmem((hidden, cols), bf16), vmem((cols, hidden), bf16)]
    scratch += [vmem((total, hidden), bf16)] * 2 + [vmem((total, cols), f32)] + [vmem((total, cols), bf16)] * 2
    scratch += [vmem((rows, cols), f32), vmem((hidden, cols), f32), vmem((cols, hidden), f32)]
    scratch += scatter_scratch(rows, hidden) * 2 + sems(AG_SEMS) * 2 + sems(RS_SEMS) * 2 + sems(11)[:1]
    outs = [((rows, hidden), False, f32)] * 2 + [(w1.shape, False, f32), (w2.shape, False, f32), ((rows, hidden), False, bf16)]
    kernel = functools.partial(mlp_kernel, layer, u is None, len(held))
    given = () if u is None else (u,)
    return call(kernel, outs, scratch, 2 * layer, "mlp_block", 12 * total * hidden * cols, 67043328, (y1, dy2, y2, dy1, w1, w2, *given), held)


def attn_block(layer, scale, u, x2, dy1, y1, dy2, wqkv, wo, held):
    rows, hidden = x2.shape
    _, heads, _, head, _ = wqkv.shape
    width = heads * head
    total = 8 * rows
    scratch = [vmem((rows, hidden), f32)] * 2 + [vmem((rows, hidden), bf16)]
    scratch += [vmem((rows, hidden), f32), vmem((heads, 3, head, hidden), f32), vmem((width, hidden), f32)] + [vmem((width, hidden), bf16)] * 3 + [vmem((8 * width, hidden), bf16)] + [vmem((total, hidden), bf16)] * 2
    scratch += [vmem((total, width), bf16)] * 5 + [vmem((8, rows * width // 128, 128), bf16)] * 2
    scratch += [vmem((8, rows, width), bf16), vmem((4, rows * width // 256, 128), bf16), vmem((16, 256, 256), f32)]
    scratch += scatter_scratch(rows // 2, hidden) * 2 + sems(AG_SEMS) * 3 + sems(13) + sems(RS_SEMS) * 2 + sems(20)[:1]
    outs = [((rows, hidden), False, f32)] * 2 + [(wqkv.shape, False, f32), (wo.shape, False, f32)]
    outs += [] if layer == 0 else [((rows, hidden), False, bf16)]
    kernel = functools.partial(attn_kernel, layer, scale, layer == 0, len(held))
    return call(kernel, outs, scratch, 2 * layer + 1, "attn_block", 24 * total * hidden * width, 67043328, (x2, dy1, y1, dy2, wqkv, wo, u), held)


def local_backward(y_one, y_two, dy_one, dy_two, w_qkv, w_out, w_up, w_down):
    n_layers, hidden, heads, _, head_dim = w_qkv.shape
    state_shape = y_one.shape
    y_one, y_two, dy_one, dy_two = [x.reshape(-1, hidden) for x in (y_one, y_two, dy_one, dy_two)]
    w_qkv = w_qkv.transpose(0, 2, 3, 4, 1)
    w_out = w_out.reshape(n_layers, heads * head_dim, hidden)
    held_mlp, held_attn, u_next = (), (), (None,)
    for layer in reversed(range(n_layers)):
        y_two, dy_one, d_up, d_down, u_att = mlp_block(
            layer, *u_next, y_one, dy_two, y_two, dy_one, w_up, w_down, held_mlp)
        held_mlp = (d_up, d_down)
        y_one, dy_two, d_qkv, d_out, *u_next = attn_block(
            layer, head_dim ** -0.5, u_att, y_two, dy_one, y_one, dy_two, w_qkv, w_out, held_attn)
        held_attn = (d_qkv, d_out)
    state = [x.reshape(state_shape) for x in (y_one, y_two, dy_one, dy_two)]
    return (*state, d_qkv.transpose(0, 4, 1, 2, 3), d_out.reshape(n_layers, heads, head_dim, hidden), d_up, d_down)


def solution(mesh):
    state_spec = P("dp", "tp", None)
    in_specs = (state_spec, state_spec, state_spec, state_spec, P(None, None, "tp", None, None), P(None, "tp", None, None), P(None, None, "tp"), P(None, "tp", None))
    out_specs = (state_spec, state_spec, state_spec, state_spec, P("dp", None, "tp", None, None), P("dp", "tp", None, None), P("dp", None, "tp"), P("dp", "tp", None))
    return jax.shard_map(local_backward, mesh=mesh, in_specs=in_specs, out_specs=out_specs, check_vma=False)
```
